512 devices in a mesh: groups: 2 (over y), tp: 8 (over x, core), sp: 32 (over z).
Axes of the slice: x: 4, y: 2, z: 32, core: 2. Of those that a mesh axis runs over, the one named last changes fastest.
The devices are a block of a 4x8x32 slice.
Arguments:
- query_rows: bfloat16 [4, 2048, 4096], P('groups', ('sp', 'tp')), parts along dimension 0, may hold values from -100 to 100
- key_rows: bfloat16 [4, 2048, 4096], P('groups', ('sp', 'tp')), parts along dimension 0, may hold values from -4 to 4
- value_rows: bfloat16 [4, 2048, 4096], P('groups', ('sp', 'tp')), parts along dimension 0, may hold values from -6 to 6
- residual: bfloat16 [4, 2048, 2560], P('groups', 'sp', 'tp'), parts along dimension 0, may hold values from -100 to 100
- modulation: float32 [4, 2560], P(None, 'tp'), may hold values from -3 to 3
- out_weight: bfloat16 [2560, 4096], P('tp', 'sp'), may hold values from -0.375 to 0.375
- up_weight: bfloat16 [2560, 7168], P('sp', 'tp'), may hold values from -0.125 to 0.125
- down_weight: bfloat16 [2560, 7168], P('sp', 'tp'), may hold values from -0.0625 to 0.0625
Outputs:
- block_out: bfloat16 [4, 2048, 2560], P('groups', 'sp', 'tp'), parts along dimension 0
The draws below stay inside these ranges and needn't reach their ends.
There are 2 independent parts, one for each index of `groups`. The reference program is written for one: setup_inputs(seed, part) draws one part's arguments, and reference() takes and returns one part's arrays. A program takes and returns all parts, laid end to end along the dimension named above; an argument that names none is the same for every part. Nothing has to cross between parts.
All inputs are finite; a program needn't handle non-finite values.
Results may differ from the reference program's by a relative error of at most 0.0044.
Values may be sent and summed in bfloat16 or wider, within the bound.
No kernel may reach another device: no remote copies, remote signals or barrier semaphores. Data moves between devices by JAX's collectives and lax.ppermute only.
A program may use at most 64 MiB of HBM per device.

```python
import math
import jax
import jax.numpy as jnp
from jax import lax

D = 2560
HEADS = 32
HEAD_FEATURES = 128
FF = 7168
MB = 2
INNER = 4096
SEQ = 2048


def attention_inputs(key):
    base_key = jax.random.fold_in(key, 7)
    key_one, key_two = jax.random.split(base_key, 2)
    keys_drawn = jax.random.truncated_normal(key_one, -4.0, 4.0, (MB, SEQ, INNER), jnp.float32)
    queries = 2.0 * jax.random.truncated_normal(key_two, -4.0, 4.0, (MB, SEQ, INNER), jnp.float32)
    keys_final = keys_drawn
    return (queries, keys_final)


def draw_query_rows(key, part):
    return attention_inputs(key)[0].astype(jnp.bfloat16)


def draw_key_rows(key, part):
    return attention_inputs(key)[1].astype(jnp.bfloat16)


def draw_residual(key, part):
    base_key = jax.random.fold_in(key, 29)
    key_one, key_two = jax.random.split(base_key, 2)
    rising = jnp.exp(jnp.linspace(0.0, math.log(3.0), D, dtype=jnp.float32))
    roughness = jnp.exp(jax.random.uniform(key_one, (D,), jnp.float32, -0.35, 0.35))
    columns = rising * roughness
    column_offset = 1.5 * rising
    drawn = jax.random.truncated_normal(key_two, -4.0, 4.0, (MB, SEQ, D), jnp.float32) * columns + column_offset
    return drawn.astype(jnp.bfloat16)


def steps_of(key, dims, pieces, low, high):
    loudness, own = 1.0, jax.random.fold_in(key, 6)
    for axis_at, shards_of in pieces:
        draws = jnp.exp(jax.random.uniform(jax.random.fold_in(own, axis_at), (shards_of,), jnp.float32, low / len(pieces), high / len(pieces)))
        loudness = loudness * jnp.repeat(draws, dims[axis_at] // shards_of).reshape([-1 if axis == axis_at else 1 for axis in range(len(dims))])
    return loudness


def noise(own_key, shape, scale, most, cuts=(), kind=jnp.bfloat16):
    level = steps_of(own_key, shape, cuts, -0.22, 0.18) if cuts else 1.0
    values = jax.random.normal(own_key, shape, jnp.float32) * scale * level
    return jnp.minimum(jnp.maximum(values, -most), most).astype(kind)


def setup_inputs(seed: int = 0, part: int = 0) -> dict:
    streams_of = jax.random.split(jax.random.key(seed), 9)
    own_keys = jax.random.split(jax.random.fold_in(streams_of[8], part), 9)
    query_rows = draw_query_rows(jax.random.fold_in(jax.random.fold_in(streams_of[8], part), 71), part)
    key_rows = draw_key_rows(jax.random.fold_in(jax.random.fold_in(streams_of[8], part), 71), part)
    value_rows = noise(own_keys[2], (MB, SEQ, INNER), 1.0, 6.0, ((1, 256),))
    residual = draw_residual(jax.random.fold_in(jax.random.fold_in(streams_of[8], part), 71), part)
    modulation = noise(streams_of[4], (4, D), 0.6, 3.0, ((1, 8),), jnp.float32)
    out_weight = noise(streams_of[5], (D, INNER), (INNER // 16) ** -0.5, 0.375, ((0, 8), (1, 32)))
    up_weight = noise(streams_of[6], (D, FF), D ** -0.5, 0.125, ((0, 32), (1, 8)))
    down_weight = noise(streams_of[7], (D, FF), FF ** -0.5, 0.0625, ((0, 32), (1, 8)))
    return dict(query_rows=query_rows, key_rows=key_rows, value_rows=value_rows, residual=residual, modulation=modulation, out_weight=out_weight, up_weight=up_weight, down_weight=down_weight)


def one_head(blocks):
    block_queries, block_keys, block_values = blocks
    attention_logits = jnp.einsum('rzs,ros->rzo', block_queries.astype(jnp.float32), block_keys.astype(jnp.float32)) / math.sqrt(HEAD_FEATURES)
    highest = lax.optimization_barrier(jnp.max(attention_logits, axis=-1, keepdims=True))
    exponent = jnp.exp(attention_logits - highest)
    row_total = lax.optimization_barrier(jnp.sum(exponent, axis=-1, keepdims=True))
    attention_weights = exponent.astype(jnp.bfloat16)
    weighted_values = jnp.einsum('ezh,ehu->ezu', attention_weights.astype(jnp.float32), block_values.astype(jnp.float32))
    return (weighted_values / row_total).astype(jnp.bfloat16)

def split_heads(packed):
    return jnp.transpose(packed.reshape(MB, SEQ, HEADS, HEAD_FEATURES), (2, 0, 1, 3))

def reference(query_rows, key_rows, value_rows, residual, modulation, out_weight, up_weight, down_weight):
    heads_out = lax.map(one_head, (split_heads(query_rows), split_heads(key_rows), split_heads(value_rows)))
    attended = jnp.transpose(heads_out, (1, 2, 0, 3)).reshape(MB * SEQ, INNER)
    projected = jnp.dot(attended, out_weight.T, preferred_element_type=jnp.float32)
    mixed_rows = residual.reshape(MB * SEQ, D).astype(jnp.float32) + modulation[0] * projected
    row_mean = lax.optimization_barrier(jnp.mean(mixed_rows, axis=1, keepdims=True))
    spread = lax.optimization_barrier(jnp.mean(jnp.square(mixed_rows - row_mean), axis=1, keepdims=True))
    normed = ((mixed_rows - row_mean) * lax.rsqrt(spread + 1e-06) * (1.0 + modulation[2]) + modulation[1]).astype(jnp.bfloat16)
    hidden = jnp.dot(normed, up_weight, preferred_element_type=jnp.float32)
    active = jax.nn.gelu(hidden, approximate=True).astype(jnp.bfloat16)
    down_out = jnp.dot(active, down_weight.T, preferred_element_type=jnp.float32)
    return (mixed_rows + modulation[3] * down_out).astype(jnp.bfloat16).reshape(MB, SEQ, D)
```

```python
import math

import jax
import jax.numpy as jnp
from jax import lax
from jax.sharding import Mesh, PartitionSpec as P

D = 2560
HEAD_FEATURES = 128
LANES = 128
CORES = 2


def contract_last(left, right):
    return lax.dot_general(
        left, right, (((1,), (1,)), ((), ())), preferred_element_type=jnp.float32
    )


def sent_to_all(array, axis):
    copies = jnp.broadcast_to(array, (lax.axis_size(axis), *array.shape))
    return lax.all_to_all(copies, axis, split_axis=0, concat_axis=0, tiled=True)


def gathered_weights(out_weight, up_weight, down_weight):
    groups = lax.axis_size("groups")
    depth, units = up_weight.shape
    pieces = [
        out_weight,
        jnp.swapaxes(up_weight.reshape(depth, units // LANES, LANES), 0, 1).reshape(-1, LANES),
        jnp.swapaxes(down_weight.reshape(depth, units // LANES, LANES), 0, 1).reshape(-1, LANES),
    ]
    packed = jnp.concatenate(pieces, axis=0)
    rows = packed.shape[0]
    chunk = -(-rows // (8 * groups)) * 8
    packed = jnp.pad(packed, ((0, chunk * groups - rows), (0, 0)))
    mine = lax.dynamic_slice_in_dim(packed, lax.axis_index("groups") * chunk, chunk, axis=0)
    everything = lax.all_gather(mine, ("groups", "sp"), axis=0, tiled=False)
    return everything.reshape(groups, lax.axis_size("sp"), chunk, LANES)


def rows_of(everything, start, stop):
    groups, _, chunk, _ = everything.shape
    parts = []
    for g in range(groups):
        low, high = max(start, g * chunk), min(stop, (g + 1) * chunk)
        if low < high:
            parts.append(everything[g, :, low - g * chunk : high - g * chunk])
    return parts[0] if len(parts) == 1 else jnp.concatenate(parts, axis=1)


def attend(query_part, key_part, value_part):
    sp = lax.axis_size("sp")
    batches, rows, width = query_part.shape
    heads = width // HEAD_FEATURES
    both = jnp.stack([query_part, key_part, value_part], axis=1)
    both = both.reshape(batches, 3, rows, heads, HEAD_FEATURES).transpose(0, 3, 1, 2, 4)
    swapped = lax.all_to_all(both, "core", split_axis=0, concat_axis=0, tiled=True)
    to_heads = jnp.swapaxes(swapped, 0, 1).reshape(sp, CORES * 3 * rows, HEAD_FEATURES)
    here = lax.all_to_all(to_heads, "sp", split_axis=0, concat_axis=0, tiled=True)
    here = here.reshape(sp, CORES, 3, rows, HEAD_FEATURES)
    count = sp * CORES * rows
    queries = here[:, :, 0].reshape(count, HEAD_FEATURES)
    own = here[:, :, 1:].transpose(2, 0, 1, 3, 4).reshape(2, count, HEAD_FEATURES)
    gathered = sent_to_all(own, "x")
    keys = gathered[:, 0].reshape(-1, HEAD_FEATURES)
    values = gathered[:, 1].reshape(-1, HEAD_FEATURES)
    scores = contract_last(queries, keys) * (1.0 / math.sqrt(HEAD_FEATURES))
    exponent = jnp.exp(scores - jnp.max(scores, axis=-1, keepdims=True))
    row_total = jnp.sum(exponent, axis=-1, keepdims=True)
    weighted = jnp.dot(
        exponent.astype(jnp.bfloat16), values, preferred_element_type=jnp.float32
    )
    attended = (weighted / row_total).astype(jnp.bfloat16)
    back = attended.reshape(sp, CORES * rows, HEAD_FEATURES)
    return lax.all_to_all(back, "sp", split_axis=0, concat_axis=0, tiled=True)


def body(
    query_rows, key_rows, value_rows, residual, modulation, out_weight, up_weight, down_weight
):
    everything = gathered_weights(out_weight, up_weight, down_weight)
    sp = lax.axis_size("sp")
    tp = ("x", "core")
    tp_size = lax.axis_size(tp)
    batches, rows_block, local_width = residual.shape
    row_count = batches * rows_block
    rows = query_rows.shape[1]
    units = up_weight.shape[1]
    depth = up_weight.shape[0]
    outs = out_weight.shape[0]

    own = attend(query_rows, key_rows, value_rows)
    stripes = sent_to_all(own, tp)
    stripes = stripes.reshape(tp_size // CORES, CORES, sp, CORES * rows, HEAD_FEATURES)
    flat_rows = stripes.transpose(1, 0, 3, 2, 4).reshape(row_count, sp * HEAD_FEATURES)

    out_full = rows_of(everything, 0, outs)
    out_full = jnp.swapaxes(out_full, 0, 1).reshape(outs, sp * LANES)
    projected = contract_last(flat_rows, out_full)
    mixed_rows = (
        residual.reshape(row_count, local_width).astype(jnp.float32) + modulation[0] * projected
    )
    sums = jnp.stack([jnp.sum(mixed_rows, axis=1), jnp.sum(mixed_rows * mixed_rows, axis=1)])
    first_sum, second_sum = jnp.sum(sent_to_all(sums, tp), axis=0)
    row_mean = first_sum / D
    spread = second_sum / D - row_mean * row_mean
    normed = (
        (mixed_rows - row_mean[:, None])
        * lax.rsqrt(spread[:, None] + 1e-06)
        * (1.0 + modulation[2])
        + modulation[1]
    ).astype(jnp.bfloat16)
    columns = jnp.swapaxes(sent_to_all(normed, tp), 0, 1).reshape(row_count, D)

    def unpacked(start):
        part = rows_of(everything, start, start + units // LANES * depth)
        part = part.reshape(sp, units // LANES, depth, LANES).transpose(0, 2, 1, 3)
        return part.reshape(sp * depth, units)

    up_full = unpacked(outs)
    down_full = unpacked(outs + units // LANES * depth)
    hidden = jnp.dot(columns, up_full, preferred_element_type=jnp.float32)
    active = jax.nn.gelu(hidden, approximate=True).astype(jnp.bfloat16)
    partial_out = contract_last(active, down_full).astype(jnp.bfloat16)
    shares = jnp.moveaxis(partial_out.reshape(row_count, tp_size, local_width), 1, 0)
    shares = lax.all_to_all(shares, tp, 0, 0, tiled=True)
    summed = jnp.sum(shares.astype(jnp.float32), axis=0)
    result = (mixed_rows + modulation[3] * summed).astype(jnp.bfloat16)
    return result.reshape(batches, rows_block, local_width)


def solution(mesh):
    groups, tp, sp = (mesh.shape[a] for a in ("groups", "tp", "sp"))
    fine = Mesh(
        mesh.devices.reshape(groups, tp // CORES, CORES, sp), ("groups", "x", "core", "sp")
    )
    tokens, tensor = ("sp", "x", "core"), ("x", "core")
    in_specs = (
        P("groups", tokens, None),
        P("groups", tokens, None),
        P("groups", tokens, None),
        P("groups", "sp", tensor),
        P(None, tensor),
        P(tensor, "sp"),
        P("sp", tensor),
        P("sp", tensor),
    )
    out_specs = P("groups", "sp", tensor)
    return jax.shard_map(body, mesh=fine, in_specs=in_specs, out_specs=out_specs, check_vma=False)
```

```python
import math

import jax
import jax.numpy as jnp
from jax import lax
from jax.sharding import Mesh, PartitionSpec as P

D = 2560
HEAD_FEATURES = 128
LANES = 128
CORES = 2


def contract_last(left, right):
    return lax.dot_general(
        left, right, (((1,), (1,)), ((), ())), preferred_element_type=jnp.float32
    )


def sent_to_all(array, axis):
    copies = jnp.broadcast_to(array, (lax.axis_size(axis), *array.shape))
    return lax.all_to_all(copies, axis, split_axis=0, concat_axis=0, tiled=True)


def gathered_weights(out_weight, up_weight, down_weight):
    depth, units = up_weight.shape
    packed = jnp.concatenate(
        [
            out_weight.reshape(-1, depth, LANES),
            jnp.swapaxes(up_weight.reshape(depth, units // LANES, LANES), 0, 1),
            jnp.swapaxes(down_weight.reshape(depth, units // LANES, LANES), 0, 1),
        ],
        axis=0,
    )
    return lax.all_gather(packed, "sp", axis=1, tiled=True)


def in_two(array):
    high = lax.reduce_precision(array, 8, 7)
    low = lax.reduce_precision(array - high, 8, 7)
    return high, low


def attend(query_part, key_part, value_part):
    sp = lax.axis_size("sp")
    batches, rows, width = query_part.shape
    heads = width // HEAD_FEATURES
    both = jnp.stack([query_part, key_part, value_part], axis=1)
    both = both.reshape(batches, 3, rows, heads, HEAD_FEATURES).transpose(0, 3, 1, 2, 4)
    swapped = lax.all_to_all(both, "core", split_axis=0, concat_axis=0, tiled=True)
    to_heads = jnp.swapaxes(swapped, 0, 1).reshape(sp, CORES * 3 * rows, HEAD_FEATURES)
    here = lax.all_to_all(to_heads, "sp", split_axis=0, concat_axis=0, tiled=True)
    here = here.reshape(sp, CORES, 3, rows, HEAD_FEATURES)
    count = sp * CORES * rows
    queries = here[:, :, 0].reshape(count, HEAD_FEATURES)
    own = here[:, :, 1:].transpose(2, 0, 1, 3, 4).reshape(2, count, HEAD_FEATURES)
    gathered = sent_to_all(own, "x")
    keys = gathered[:, 0].reshape(-1, HEAD_FEATURES)
    values = gathered[:, 1].reshape(-1, HEAD_FEATURES)
    scores = contract_last(queries, keys) * (1.0 / math.sqrt(HEAD_FEATURES))
    exponent = jnp.exp(scores - jnp.max(scores, axis=-1, keepdims=True))
    row_total = jnp.sum(exponent, axis=-1, keepdims=True)
    weighted = jnp.dot(
        exponent.astype(jnp.bfloat16), values, preferred_element_type=jnp.float32
    )
    attended = (weighted / row_total).astype(jnp.bfloat16)
    back = attended.reshape(sp, CORES * rows, HEAD_FEATURES)
    return lax.all_to_all(back, "sp", split_axis=0, concat_axis=0, tiled=True)


def body(
    query_rows, key_rows, value_rows, residual, modulation, out_weight, up_weight, down_weight
):
    everything = gathered_weights(out_weight, up_weight, down_weight)
    sp = lax.axis_size("sp")
    tp = ("x", "core")
    tp_size = lax.axis_size(tp)
    batches, rows_block, local_width = residual.shape
    row_count = batches * rows_block
    rows = query_rows.shape[1]
    depth, units = up_weight.shape
    out_pieces, unit_pieces = local_width // depth, units // LANES

    own = attend(query_rows, key_rows, value_rows)
    own = own.reshape(-1, HEAD_FEATURES)
    shift_scale = jnp.stack(in_two(modulation[1:3])).astype(jnp.bfloat16).reshape(-1, LANES)
    extra = -shift_scale.shape[0] % 16
    message = jnp.concatenate([own, jnp.pad(shift_scale, ((0, extra), (0, 0)))], axis=0)
    stripes = sent_to_all(message, tp)
    halves = stripes[:, own.shape[0] : own.shape[0] + shift_scale.shape[0]]
    halves = halves.reshape(tp_size, 2, 2, local_width).astype(jnp.float32)
    shift, scale = (halves[:, 0, k] + halves[:, 1, k] for k in range(2))
    stripes = stripes[:, : own.shape[0]].reshape(
        tp_size // CORES, CORES, sp, CORES * rows, HEAD_FEATURES
    )
    flat_rows = stripes.transpose(1, 0, 3, 2, 4).reshape(row_count, sp, HEAD_FEATURES)

    out_full = everything[:out_pieces].reshape(out_pieces, sp, depth, LANES)
    projected = jnp.einsum(
        "rsf,psif->rpi", flat_rows, out_full, preferred_element_type=jnp.float32
    ).reshape(row_count, local_width)
    mixed_rows = (
        residual.reshape(row_count, local_width).astype(jnp.float32) + modulation[0] * projected
    )
    high, low = in_two(jnp.mean(mixed_rows, axis=1, keepdims=True))
    deviation = mixed_rows - (high + low)
    message = jnp.concatenate(
        [deviation, high, low, jnp.zeros((row_count, 14), jnp.float32)], axis=1
    ).astype(jnp.bfloat16)
    spreads = sent_to_all(message, tp).astype(jnp.float32)
    spreads = (
        spreads[:, :, :local_width]
        + spreads[:, :, local_width : local_width + 1]
        + spreads[:, :, local_width + 1 : local_width + 2]
    )
    row_mean = jnp.mean(spreads, axis=(0, 2), keepdims=True)
    centred = spreads - row_mean
    spread = jnp.mean(centred * centred, axis=(0, 2), keepdims=True)
    normed = (
        centred * lax.rsqrt(spread + 1e-06) * (1.0 + scale[:, None]) + shift[:, None]
    ).astype(jnp.bfloat16)
    columns = jnp.swapaxes(normed, 0, 1).reshape(row_count, D)

    up_full = everything[out_pieces : out_pieces + unit_pieces]
    down_full = everything[out_pieces + unit_pieces :]
    hidden = jnp.einsum("rk,jkn->rjn", columns, up_full, preferred_element_type=jnp.float32)
    active = jax.nn.gelu(hidden, approximate=True).astype(jnp.bfloat16)
    partial_out = jnp.einsum(
        "rjn,jon->ro", active, down_full, preferred_element_type=jnp.float32
    ).astype(jnp.bfloat16)
    shares = jnp.moveaxis(partial_out.reshape(row_count, tp_size, local_width), 1, 0)
    shares = lax.all_to_all(shares, tp, 0, 0, tiled=True)
    summed = jnp.sum(shares.astype(jnp.float32), axis=0)
    result = (mixed_rows + modulation[3] * summed).astype(jnp.bfloat16)
    return result.reshape(batches, rows_block, local_width)


def solution(mesh):
    groups, tp, sp = (mesh.shape[a] for a in ("groups", "tp", "sp"))
    fine = Mesh(
        mesh.devices.reshape(groups, tp // CORES, CORES, sp), ("groups", "x", "core", "sp")
    )
    tokens, tensor = ("sp", "x", "core"), ("x", "core")
    in_specs = (
        P("groups", tokens, None),
        P("groups", tokens, None),
        P("groups", tokens, None),
        P("groups", "sp", tensor),
        P(None, tensor),
        P(tensor, "sp"),
        P("sp", tensor),
        P("sp", tensor),
    )
    out_specs = P("groups", "sp", tensor)
    return jax.shard_map(body, mesh=fine, in_specs=in_specs, out_specs=out_specs, check_vma=False)
```

```python
import functools
import math

import jax
import jax.numpy as jnp
from jax import lax
from jax.experimental import pallas as pl
from jax.experimental.pallas import tpu as pltpu
from jax.sharding import Mesh, PartitionSpec as P

HEAD_FEATURES = 128
LANES = 128
CORES = 2
MEBI = 1 << 20
LIMIT = 48


def contract_last(left, right):
    return lax.dot_general(
        left, right, (((1,), (1,)), ((), ())), preferred_element_type=jnp.float32
    )


def sent_to_all(array, axis):
    copies = jnp.broadcast_to(array, (lax.axis_size(axis), *array.shape))
    return lax.all_to_all(copies, axis, split_axis=0, concat_axis=0, tiled=True)


def gathered_weights(out_weight, up_weight, down_weight):
    depth, units = up_weight.shape
    packed = jnp.concatenate(
        [
            out_weight,
            jnp.swapaxes(up_weight.reshape(depth, units // LANES, LANES), 0, 1).reshape(-1, LANES),
            jnp.swapaxes(down_weight.reshape(depth, units // LANES, LANES), 0, 1).reshape(-1, LANES),
        ],
        axis=0,
    )
    return lax.all_gather(packed, "sp", axis=0, tiled=False)


def in_two(array):
    high = lax.reduce_precision(array, 8, 7)
    low = lax.reduce_precision(array - high, 8, 7)
    return high, low


def attend(query_part, key_part, value_part):
    sp = lax.axis_size("sp")
    batches, rows, width = query_part.shape
    heads = width // HEAD_FEATURES
    both = jnp.stack([query_part, key_part, value_part], axis=1)
    both = both.reshape(batches, 3, rows, heads, HEAD_FEATURES).transpose(0, 3, 1, 2, 4)
    swapped = lax.all_to_all(both, "core", split_axis=0, concat_axis=0, tiled=True)
    to_heads = jnp.swapaxes(swapped, 0, 1).reshape(sp, CORES * 3 * rows, HEAD_FEATURES)
    here = lax.all_to_all(to_heads, "sp", split_axis=0, concat_axis=0, tiled=True)
    here = here.reshape(sp, CORES, 3, rows, HEAD_FEATURES)
    count = sp * CORES * rows
    queries = here[:, :, 0].reshape(count, HEAD_FEATURES)
    own = here[:, :, 1:].transpose(2, 0, 1, 3, 4).reshape(2, count, HEAD_FEATURES)
    gathered = sent_to_all(own, "x")
    keys = gathered[:, 0].reshape(-1, HEAD_FEATURES)
    values = gathered[:, 1].reshape(-1, HEAD_FEATURES)
    scores = contract_last(queries, keys) * (1.0 / math.sqrt(HEAD_FEATURES))
    exponent = jnp.exp(scores - jnp.max(scores, axis=-1, keepdims=True))
    row_total = jnp.sum(exponent, axis=-1, keepdims=True)
    weighted = jnp.dot(
        exponent.astype(jnp.bfloat16), values, preferred_element_type=jnp.float32
    )
    attended = (weighted / row_total).astype(jnp.bfloat16)
    back = attended.reshape(sp, CORES * rows, HEAD_FEATURES)
    return lax.all_to_all(back, "sp", split_axis=0, concat_axis=0, tiled=True)


def project_kernel(
    parts, stripes_ref, weights_ref, residual_ref, modulation_ref, mixed_ref, message_ref, held, sems
):
    heads, outs, _ = held.shape
    tp_size = stripes_ref.shape[0]
    each = heads // parts
    copies = [
        pltpu.make_async_copy(
            weights_ref.at[pl.ds(k * each, each), pl.ds(0, outs), :],
            held.at[pl.ds(k * each, each)],
            sems.at[k],
        )
        for k in range(parts)
    ]
    for copy in copies:
        copy.start()
    batches, rows_block, _ = residual_ref.shape
    span = batches * rows_block // tp_size
    residual = jnp.concatenate(
        [
            residual_ref[t % batches, t // batches * span : (t // batches + 1) * span, :]
            for t in range(tp_size)
        ],
        axis=0,
    ).astype(jnp.float32)
    total = jnp.zeros(residual.shape, jnp.float32)
    for k in range(parts):
        copies[k].wait()
        for h in range(k * each, (k + 1) * each, 2):
            left, right = (
                jnp.concatenate(pair, axis=1)
                for pair in (
                    [
                        stripes_ref[:, i * span : (i + 1) * span, :].reshape(-1, LANES)
                        for i in (h, h + 1)
                    ],
                    [held[h], held[h + 1]],
                )
            )
            total = total + contract_last(left, right)
    mixed = residual + modulation_ref[0:1, :] * total
    mixed_ref[...] = mixed
    mean = jnp.mean(mixed, axis=1, keepdims=True)
    high = mean.astype(jnp.bfloat16)
    low = (mean - high.astype(jnp.float32)).astype(jnp.bfloat16)
    deviation = mixed - (high.astype(jnp.float32) + low.astype(jnp.float32))
    width = mixed.shape[1]
    message_ref[:, 0:width] = deviation.astype(jnp.bfloat16)
    rest = message_ref.shape[1] - width
    lane = lax.broadcasted_iota(jnp.int32, (mixed.shape[0], rest), 1)
    message_ref[:, width:] = jnp.where(
        lane == 0, high.astype(jnp.float32), jnp.where(lane == 1, low.astype(jnp.float32), 0.0)
    ).astype(jnp.bfloat16)


def project(stripes, everything, residual, modulation):
    outs = modulation.shape[1]
    rows = residual.shape[0] * residual.shape[1]
    sp = everything.shape[0]
    parts = 4
    vmem = pl.BlockSpec(memory_space=pltpu.VMEM)
    return pl.pallas_call(
        functools.partial(project_kernel, parts),
        out_shape=(
            jax.ShapeDtypeStruct((rows, outs), jnp.float32),
            jax.ShapeDtypeStruct((rows, -(-(outs + 2) // LANES) * LANES), jnp.bfloat16),
        ),
        in_specs=[vmem, pl.BlockSpec(memory_space=pltpu.HBM), vmem, vmem],
        out_specs=(vmem, vmem),
        scratch_shapes=[
            pltpu.VMEM((sp, outs, LANES), jnp.bfloat16),
            pltpu.SemaphoreType.DMA((parts,)),
        ],
        compiler_params=pltpu.CompilerParams(vmem_limit_bytes=LIMIT * MEBI),
        name="project",
    )(stripes, everything, residual, modulation)


def feed_kernel(outs, messages_ref, scales_ref, weights_ref, shares_ref, ups, downs, sems):
    sp, depth, units = ups.shape
    pieces = units // LANES
    tp_size, rows, _ = messages_ref.shape
    copies = []
    for matrix, held in enumerate((ups, downs)):
        for j in range(pieces):
            k = matrix * pieces + j
            copies.append(
                pltpu.make_async_copy(
                    weights_ref.at[:, pl.ds(outs + k * depth, depth), :],
                    held.at[:, :, pl.ds(j * LANES, LANES)],
                    sems.at[k],
                )
            )
    for copy in copies:
        copy.start()
    spreads = []
    for t in range(tp_size):
        mean = messages_ref[t, :, outs : outs + 2].astype(jnp.float32)
        spreads.append(
            messages_ref[t, :, 0:outs].astype(jnp.float32) + (mean[:, 0:1] + mean[:, 1:2])
        )
    features = tp_size * outs
    row_mean = sum(jnp.sum(part, axis=1, keepdims=True) for part in spreads) / features
    centred = [part - row_mean for part in spreads]
    spread = sum(jnp.sum(part * part, axis=1, keepdims=True) for part in centred) / features
    factor = lax.rsqrt(spread + 1e-06)
    normed = jnp.concatenate(
        [
            centred[t] * factor * (1.0 + scales_ref[1, t : t + 1, :]) + scales_ref[0, t : t + 1, :]
            for t in range(tp_size)
        ],
        axis=1,
    ).astype(jnp.bfloat16)
    active = []
    for j in range(0, pieces, 2):
        stop = min(j + 2, pieces)
        for k in range(j, stop):
            copies[k].wait()
        block = ups[:, :, j * LANES : stop * LANES].reshape(sp * depth, -1)
        hidden = jnp.dot(normed, block, preferred_element_type=jnp.float32)
        active.append(jax.nn.gelu(hidden, approximate=True).astype(jnp.bfloat16))
    active = jnp.concatenate(active, axis=1)
    for copy in copies[pieces:]:
        copy.wait()
    each = sp // tp_size
    for t in range(tp_size):
        block = downs[t * each : (t + 1) * each].reshape(each * depth, units)
        shares_ref[t] = contract_last(block, active).astype(jnp.bfloat16)


def feed(messages, scales, everything, depth, units):
    tp_size, rows, _ = messages.shape
    outs = scales.shape[2]
    sp = everything.shape[0]
    vmem = pl.BlockSpec(memory_space=pltpu.VMEM)
    return pl.pallas_call(
        functools.partial(feed_kernel, outs),
        out_shape=jax.ShapeDtypeStruct((tp_size, outs, rows), jnp.bfloat16),
        in_specs=[vmem, vmem, pl.BlockSpec(memory_space=pltpu.HBM)],
        out_specs=vmem,
        scratch_shapes=[
            pltpu.VMEM((sp, depth, units), jnp.bfloat16),
            pltpu.VMEM((sp, depth, units), jnp.bfloat16),
            pltpu.SemaphoreType.DMA((2 * units // LANES,)),
        ],
        compiler_params=pltpu.CompilerParams(vmem_limit_bytes=LIMIT * MEBI),
        name="feed",
    )(messages, scales, everything)


def finish_kernel(shares_ref, mixed_ref, modulation_ref, out_ref):
    tp_size, outs, rows = shares_ref.shape
    batches = out_ref.shape[0]
    span = rows // tp_size
    total = jnp.zeros((outs, rows), jnp.float32)
    for t in range(tp_size):
        total = total + shares_ref[t].astype(jnp.float32)
    rest = -outs % LANES
    turned = jnp.concatenate([total, jnp.zeros((rest, rows), jnp.float32)], axis=0).T[:, :outs]
    result = (mixed_ref[...] + modulation_ref[3:4, :] * turned).astype(jnp.bfloat16)
    for t in range(tp_size):
        place = t // batches * span
        out_ref[t % batches, place : place + span, :] = result[t * span : (t + 1) * span]


def body(
    query_rows, key_rows, value_rows, residual, modulation, out_weight, up_weight, down_weight
):
    everything = gathered_weights(out_weight, up_weight, down_weight)
    tp = ("x", "core")
    tp_size = lax.axis_size(tp)
    local_width = residual.shape[2]
    depth, units = up_weight.shape

    own = attend(query_rows, key_rows, value_rows)
    own = own.reshape(-1, HEAD_FEATURES)
    shift_scale = jnp.stack(in_two(modulation[1:3])).astype(jnp.bfloat16).reshape(-1, LANES)
    extra = -shift_scale.shape[0] % 16
    message = jnp.concatenate([own, jnp.pad(shift_scale, ((0, extra), (0, 0)))], axis=0)
    stripes = sent_to_all(message, tp)
    halves = stripes[:, own.shape[0] : own.shape[0] + shift_scale.shape[0]]
    halves = halves.reshape(tp_size, 2, 2, local_width).astype(jnp.float32)
    scales = jnp.swapaxes(halves[:, 0] + halves[:, 1], 0, 1)

    mixed, message = project(stripes, everything, residual, modulation)
    messages = lax.all_gather(message, tp, axis=0, tiled=False)
    shares = feed(messages, scales, everything, depth, units)
    shares = lax.all_to_all(shares, tp, 0, 0, tiled=True)
    return pl.pallas_call(
        finish_kernel,
        out_shape=jax.ShapeDtypeStruct(residual.shape, residual.dtype),
        compiler_params=pltpu.CompilerParams(vmem_limit_bytes=8 * MEBI),
        name="finish",
    )(shares, mixed, modulation)


def solution(mesh):
    groups, tp, sp = (mesh.shape[a] for a in ("groups", "tp", "sp"))
    fine = Mesh(
        mesh.devices.reshape(groups, tp // CORES, CORES, sp), ("groups", "x", "core", "sp")
    )
    tokens, tensor = ("sp", "x", "core"), ("x", "core")
    in_specs = (
        P("groups", tokens, None),
        P("groups", tokens, None),
        P("groups", tokens, None),
        P("groups", "sp", tensor),
        P(None, tensor),
        P(tensor, "sp"),
        P("sp", tensor),
        P("sp", tensor),
    )
    out_specs = P("groups", "sp", tensor)
    return jax.shard_map(body, mesh=fine, in_specs=in_specs, out_specs=out_specs, check_vma=False)
```

```python
import functools
import math

import jax
import jax.numpy as jnp
from jax import lax
from jax.experimental import pallas as pl
from jax.experimental.pallas import tpu as pltpu
from jax.sharding import Mesh, PartitionSpec as P

HEAD_FEATURES = 128
LANES = 128
CORES = 2
MEBI = 1 << 20
LIMIT = 48
MEAN_PARTS = 3


def contract_last(left, right):
    return lax.dot_general(
        left, right, (((1,), (1,)), ((), ())), preferred_element_type=jnp.float32
    )


def sent_to_all(array, axis):
    copies = jnp.broadcast_to(array, (lax.axis_size(axis), *array.shape))
    return lax.all_to_all(copies, axis, split_axis=0, concat_axis=0, tiled=True)


def gathered_weights(out_weight, up_weight, down_weight):
    depth, units = up_weight.shape
    packed = jnp.concatenate(
        [
            out_weight,
            jnp.swapaxes(up_weight.reshape(depth, units // LANES, LANES), 0, 1).reshape(-1, LANES),
            jnp.swapaxes(down_weight.reshape(depth, units // LANES, LANES), 0, 1).reshape(-1, LANES),
        ],
        axis=0,
    )
    return lax.all_gather(packed, "sp", axis=0, tiled=False)


def in_two(array):
    high = lax.reduce_precision(array, 8, 7)
    low = lax.reduce_precision(array - high, 8, 7)
    return high, low


def attend(query_part, key_part, value_part):
    sp = lax.axis_size("sp")
    batches, rows, width = query_part.shape
    heads = width // HEAD_FEATURES
    both = jnp.stack([query_part, key_part, value_part], axis=1)
    both = both.reshape(batches, 3, rows, heads, HEAD_FEATURES).transpose(0, 3, 1, 2, 4)
    swapped = lax.all_to_all(both, "core", split_axis=0, concat_axis=0, tiled=True)
    to_heads = jnp.swapaxes(swapped, 0, 1).reshape(sp, CORES * 3 * rows, HEAD_FEATURES)
    here = lax.all_to_all(to_heads, "sp", split_axis=0, concat_axis=0, tiled=True)
    here = here.reshape(sp, CORES, 3, rows, HEAD_FEATURES)
    count = sp * CORES * rows
    queries = here[:, :, 0].reshape(count, HEAD_FEATURES)
    own = here[:, :, 1:].transpose(2, 0, 1, 3, 4).reshape(2, count, HEAD_FEATURES)
    gathered = sent_to_all(own, "x")
    keys = gathered[:, 0].reshape(-1, HEAD_FEATURES)
    values = gathered[:, 1].reshape(-1, HEAD_FEATURES)
    scores = contract_last(queries, keys) * (1.0 / math.sqrt(HEAD_FEATURES))
    exponent = jnp.exp(scores - jnp.max(scores, axis=-1, keepdims=True))
    row_total = jnp.sum(exponent, axis=-1, keepdims=True)
    weighted = jnp.dot(
        exponent.astype(jnp.bfloat16), values, preferred_element_type=jnp.float32
    )
    attended = (weighted / row_total).astype(jnp.bfloat16)
    back = attended.reshape(sp, CORES * rows, HEAD_FEATURES)
    return lax.all_to_all(back, "sp", split_axis=0, concat_axis=0, tiled=True)


def project_kernel(
    parts, stripes_ref, weights_ref, residual_ref, modulation_ref, mixed_ref, message_ref, held, sems
):
    heads, outs, _ = held.shape
    tp_size = stripes_ref.shape[0]
    each = heads // parts
    copies = [
        pltpu.make_async_copy(
            weights_ref.at[pl.ds(k * each, each), pl.ds(0, outs), :],
            held.at[pl.ds(k * each, each)],
            sems.at[k],
        )
        for k in range(parts)
    ]
    for copy in copies:
        copy.start()
    batches, rows_block, _ = residual_ref.shape
    span = batches * rows_block // tp_size
    residual = jnp.concatenate(
        [
            residual_ref[t % batches, t // batches * span : (t // batches + 1) * span, :]
            for t in range(tp_size)
        ],
        axis=0,
    ).astype(jnp.float32)
    total = jnp.zeros(residual.shape, jnp.float32)
    for k in range(parts):
        copies[k].wait()
        for h in range(k * each, (k + 1) * each, 2):
            left, right = (
                jnp.concatenate(pair, axis=1)
                for pair in (
                    [
                        stripes_ref[:, i * span : (i + 1) * span, :].reshape(-1, LANES)
                        for i in (h, h + 1)
                    ],
                    [held[h], held[h + 1]],
                )
            )
            total = total + contract_last(left, right)
    mixed = residual + modulation_ref[0:1, :] * total
    mixed_ref[...] = mixed
    mean = jnp.mean(mixed, axis=1, keepdims=True)
    left, told, places = mean, jnp.zeros_like(mean), []
    for _ in range(MEAN_PARTS):
        places.append(left.astype(jnp.bfloat16).astype(jnp.float32))
        told = told + places[-1]
        left = mean - told
    width = mixed.shape[1]
    lane = lax.broadcasted_iota(jnp.int32, (mixed.shape[0], -width % LANES), 1)
    means = jnp.zeros(lane.shape, jnp.float32)
    for k, place in enumerate(places):
        means = jnp.where(lane == k, place, means)
    turned = jnp.concatenate([mixed - told, means], axis=1).T
    message_ref[...] = turned[: message_ref.shape[0]].astype(jnp.bfloat16)


def project(stripes, everything, residual, modulation):
    outs = modulation.shape[1]
    rows = residual.shape[0] * residual.shape[1]
    sp = everything.shape[0]
    parts = 8
    vmem = pl.BlockSpec(memory_space=pltpu.VMEM)
    return pl.pallas_call(
        functools.partial(project_kernel, parts),
        out_shape=(
            jax.ShapeDtypeStruct((rows, outs), jnp.float32),
            jax.ShapeDtypeStruct((outs + 16, rows), jnp.bfloat16),
        ),
        in_specs=[vmem, pl.BlockSpec(memory_space=pltpu.HBM), vmem, vmem],
        out_specs=(vmem, vmem),
        scratch_shapes=[
            pltpu.VMEM((sp, outs, LANES), jnp.bfloat16),
            pltpu.SemaphoreType.DMA((parts,)),
        ],
        compiler_params=pltpu.CompilerParams(vmem_limit_bytes=LIMIT * MEBI),
        name="project",
    )(stripes, everything, residual, modulation)


def feed_kernel(messages_ref, scales_ref, weights_ref, shares_ref, ups, downs, sems):
    sp, depth, units = ups.shape
    pieces = units // LANES
    tp_size = messages_ref.shape[0]
    features = scales_ref.shape[1]
    outs = features // tp_size
    half = sp // 2

    def copy_of(held, k, j, start, count, sem):
        return pltpu.make_async_copy(
            weights_ref.at[pl.ds(start, count), pl.ds(outs + k * depth, depth), :],
            held.at[pl.ds(start, count), :, pl.ds(j * LANES, LANES)],
            sems.at[sem],
        )

    up_copies = [copy_of(ups, j, j, 0, sp, j) for j in range(pieces)]
    down_copies = [
        [
            copy_of(downs, pieces + j, j, side * half, half, (1 + side) * pieces + j)
            for j in range(pieces)
        ]
        for side in range(2)
    ]
    for copy in [*up_copies, *down_copies[0], *down_copies[1]]:
        copy.start()
    spreads = []
    for t in range(tp_size):
        mean = jnp.sum(
            messages_ref[t, outs : outs + 16, :].astype(jnp.float32), axis=0, keepdims=True
        )
        spreads.append(messages_ref[t, 0:outs, :].astype(jnp.float32) + mean)
    row_mean = sum(jnp.sum(part, axis=0, keepdims=True) for part in spreads) / features
    centred = [part - row_mean for part in spreads]
    spread = sum(jnp.sum(part * part, axis=0, keepdims=True) for part in centred) / features
    factor = lax.rsqrt(spread + 1e-06)
    turned = jnp.concatenate([part * factor for part in centred], axis=0).T
    normed = (turned * (1.0 + scales_ref[1:2, :]) + scales_ref[0:1, :]).astype(jnp.bfloat16)
    active = []
    for j in range(0, pieces, 2):
        stop = min(j + 2, pieces)
        for k in range(j, stop):
            up_copies[k].wait()
        block = ups[:, :, j * LANES : stop * LANES].reshape(sp * depth, -1)
        hidden = jnp.dot(normed, block, preferred_element_type=jnp.float32)
        active.append(jax.nn.gelu(hidden, approximate=True).astype(jnp.bfloat16))
    active = jnp.concatenate(active, axis=1)
    each = sp // tp_size
    for side in range(2):
        for copy in down_copies[side]:
            copy.wait()
        for t in range(side * tp_size // 2, (side + 1) * tp_size // 2):
            block = downs[t * each : (t + 1) * each].reshape(each * depth, units)
            shares_ref[t] = contract_last(block, active).astype(jnp.bfloat16)


def feed(messages, scales, everything, depth, units):
    tp_size, _, rows = messages.shape
    outs = scales.shape[1] // tp_size
    sp = everything.shape[0]
    vmem = pl.BlockSpec(memory_space=pltpu.VMEM)
    return pl.pallas_call(
        feed_kernel,
        out_shape=jax.ShapeDtypeStruct((tp_size, outs, rows), jnp.bfloat16),
        in_specs=[vmem, vmem, pl.BlockSpec(memory_space=pltpu.HBM)],
        out_specs=vmem,
        scratch_shapes=[
            pltpu.VMEM((sp, depth, units), jnp.bfloat16),
            pltpu.VMEM((sp, depth, units), jnp.bfloat16),
            pltpu.SemaphoreType.DMA((3 * units // LANES,)),
        ],
        compiler_params=pltpu.CompilerParams(vmem_limit_bytes=LIMIT * MEBI),
        name="feed",
    )(messages, scales, everything)


def finish_kernel(shares_ref, mixed_ref, modulation_ref, out_ref):
    tp_size, outs, rows = shares_ref.shape
    batches = out_ref.shape[0]
    span = rows // tp_size
    total = jnp.zeros((outs, rows), jnp.float32)
    for t in range(tp_size):
        total = total + shares_ref[t].astype(jnp.float32)
    rest = -outs % LANES
    turned = jnp.concatenate([total, jnp.zeros((rest, rows), jnp.float32)], axis=0).T[:, :outs]
    result = (mixed_ref[...] + modulation_ref[3:4, :] * turned).astype(jnp.bfloat16)
    for t in range(tp_size):
        place = t // batches * span
        out_ref[t % batches, place : place + span, :] = result[t * span : (t + 1) * span]


def body(
    query_rows, key_rows, value_rows, residual, modulation, out_weight, up_weight, down_weight
):
    everything = gathered_weights(out_weight, up_weight, down_weight)
    tp = ("x", "core")
    tp_size = lax.axis_size(tp)
    local_width = residual.shape[2]
    depth, units = up_weight.shape

    own = attend(query_rows, key_rows, value_rows)
    own = own.reshape(-1, HEAD_FEATURES)
    shift_scale = jnp.stack(in_two(modulation[1:3])).astype(jnp.bfloat16).reshape(-1, LANES)
    extra = -shift_scale.shape[0] % 16
    message = jnp.concatenate([own, jnp.pad(shift_scale, ((0, extra), (0, 0)))], axis=0)
    stripes = sent_to_all(message, tp)
    halves = stripes[:, own.shape[0] : own.shape[0] + shift_scale.shape[0]]
    halves = halves.reshape(tp_size, 2, 2, local_width).astype(jnp.float32)
    scales = jnp.swapaxes(halves[:, 0] + halves[:, 1], 0, 1).reshape(2, -1)

    mixed, message = project(stripes, everything, residual, modulation)
    messages = lax.all_gather(message, tp, axis=0, tiled=False)
    shares = feed(messages, scales, everything, depth, units)
    shares = lax.all_to_all(shares, tp, 0, 0, tiled=True)
    return pl.pallas_call(
        finish_kernel,
        out_shape=jax.ShapeDtypeStruct(residual.shape, residual.dtype),
        compiler_params=pltpu.CompilerParams(vmem_limit_bytes=8 * MEBI),
        name="finish",
    )(shares, mixed, modulation)


def solution(mesh):
    groups, tp, sp = (mesh.shape[a] for a in ("groups", "tp", "sp"))
    fine = Mesh(
        mesh.devices.reshape(groups, tp // CORES, CORES, sp), ("groups", "x", "core", "sp")
    )
    tokens, tensor = ("sp", "x", "core"), ("x", "core")
    in_specs = (
        P("groups", tokens, None),
        P("groups", tokens, None),
        P("groups", tokens, None),
        P("groups", "sp", tensor),
        P(None, tensor),
        P(tensor, "sp"),
        P("sp", tensor),
        P("sp", tensor),
    )
    out_specs = P("groups", "sp", tensor)
    return jax.shard_map(body, mesh=fine, in_specs=in_specs, out_specs=out_specs, check_vma=False)
```

```python
import functools
import math

import jax
import jax.numpy as jnp
from jax import lax
from jax.experimental import pallas as pl
from jax.experimental.pallas import tpu as pltpu
from jax.sharding import Mesh, PartitionSpec as P

HEAD_FEATURES = 128
LANES = 128
CORES = 2
PAIR = 2
MEBI = 1 << 20
LIMIT = 48
MEAN_PARTS = 3


def contract_last(left, right):
    return lax.dot_general(
        left, right, (((1,), (1,)), ((), ())), preferred_element_type=jnp.float32
    )


def sent_to_all(array, axis):
    copies = jnp.broadcast_to(array, (lax.axis_size(axis), *array.shape))
    return lax.all_to_all(copies, axis, split_axis=0, concat_axis=0, tiled=True)


def gathered_weights(out_weight, up_weight, down_weight, side):
    depth, units = up_weight.shape
    outs = out_weight.shape[0]

    def half(array, dim):
        size = array.shape[dim] // PAIR
        parts = [lax.slice_in_dim(array, k * size, (k + 1) * size, axis=dim) for k in range(PAIR)]
        return jnp.where(side == 0, parts[0], parts[1])

    up_half, down_half = half(up_weight, 1), half(down_weight, 1)
    whole = units // PAIR // LANES * LANES
    pieces = [half(out_weight, 0)]
    for matrix in (up_half, down_half):
        for start in range(0, whole, LANES):
            pieces.append(matrix[:, start : start + LANES])
    pieces.append(jnp.concatenate([up_half[:, whole:], down_half[:, whole:]], axis=1))
    packed = jnp.concatenate(pieces, axis=0)
    everything = lax.all_gather(packed, ("sp", "core"), axis=0, tiled=False)
    return everything.reshape(lax.axis_size("sp"), CORES, *packed.shape)


def attend(query_part, key_part, value_part):
    sp = lax.axis_size("sp")
    batches, rows, width = query_part.shape
    heads = width // HEAD_FEATURES
    both = jnp.stack([query_part, key_part, value_part], axis=1)
    both = both.reshape(batches, 3, rows, heads, HEAD_FEATURES).transpose(0, 3, 1, 2, 4)
    swapped = lax.all_to_all(both, "core", split_axis=0, concat_axis=0, tiled=True)
    to_heads = jnp.swapaxes(swapped, 0, 1).reshape(sp, CORES * 3 * rows, HEAD_FEATURES)
    here = lax.all_to_all(to_heads, "sp", split_axis=0, concat_axis=0, tiled=True)
    here = here.reshape(sp, CORES, 3, rows, HEAD_FEATURES)
    count = sp * CORES * rows
    queries = here[:, :, 0].reshape(count, HEAD_FEATURES)
    own = here[:, :, 1:].transpose(2, 0, 1, 3, 4).reshape(2, count, HEAD_FEATURES)
    gathered = sent_to_all(own, "x")
    keys = gathered[:, 0].reshape(-1, HEAD_FEATURES)
    values = gathered[:, 1].reshape(-1, HEAD_FEATURES)
    scores = contract_last(queries, keys) * (1.0 / math.sqrt(HEAD_FEATURES))
    exponent = jnp.exp(scores - jnp.max(scores, axis=-1, keepdims=True))
    row_total = jnp.sum(exponent, axis=-1, keepdims=True)
    weighted = jnp.dot(
        exponent.astype(jnp.bfloat16), values, preferred_element_type=jnp.float32
    )
    attended = (weighted / row_total).astype(jnp.bfloat16)
    back = attended.reshape(sp, CORES * rows, HEAD_FEATURES)
    return lax.all_to_all(back, "sp", split_axis=0, concat_axis=0, tiled=True)


def project_kernel(
    parts, place_ref, stripes_ref, weights_ref, residual_ref, gate_ref, placed_ref, message_ref, held, sems
):
    heads, _, half, _ = held.shape
    width = CORES * half
    each = heads // parts
    copies = [
        pltpu.make_async_copy(
            weights_ref.at[pl.ds(k * each, each), :, pl.ds(0, half), :],
            held.at[pl.ds(k * each, each)],
            sems.at[k],
        )
        for k in range(parts)
    ]
    for copy in copies:
        copy.start()
    sources = stripes_ref.shape[0]
    rows = residual_ref.shape[0]
    span = rows // sources
    residual = residual_ref[...].astype(jnp.float32)
    placed_ref[...] = jnp.zeros(placed_ref.shape, jnp.float32)
    total = jnp.zeros(residual.shape, jnp.float32)
    for k in range(parts):
        copies[k].wait()
        for h in range(k * each, (k + 1) * each, 2):
            left, right = (
                jnp.concatenate(pair, axis=1)
                for pair in (
                    [
                        stripes_ref[:, i * span : (i + 1) * span, :].reshape(-1, LANES)
                        for i in (h, h + 1)
                    ],
                    [held[i].reshape(width, LANES) for i in (h, h + 1)],
                )
            )
            total = total + contract_last(left, right)
    mixed = residual + gate_ref[...] * total
    mean = jnp.mean(mixed, axis=1, keepdims=True)
    left, told, columns = mean, jnp.zeros_like(mean), []
    for _ in range(MEAN_PARTS):
        columns.append(left.astype(jnp.bfloat16).astype(jnp.float32))
        told = told + columns[-1]
        left = mean - told
    lane = lax.broadcasted_iota(jnp.int32, (rows, -width % LANES), 1)
    rest = jnp.zeros(lane.shape, jnp.float32)
    for k, column in enumerate(columns):
        rest = jnp.where(lane == k, column, rest)
    rest = jnp.where(lane == 16, told, rest)
    turned = jnp.concatenate([mixed, rest], axis=1).T
    message_ref[0:width, :] = (turned[0:width] - turned[width + 16 : width + 17]).astype(
        jnp.bfloat16
    )
    message_ref[width : width + 16, :] = turned[width : width + 16].astype(jnp.bfloat16)
    at = pl.multiple_of(place_ref[1] * half, half)
    for core in range(CORES):
        placed_ref[core, pl.ds(at, half), :] = turned[core * half : (core + 1) * half]


def project(place, stripes, everything, residual, gate):
    rows, outs = residual.shape
    sp = everything.shape[0]
    parts = 8
    vmem = pl.BlockSpec(memory_space=pltpu.VMEM)
    smem = pl.BlockSpec(memory_space=pltpu.SMEM)
    return pl.pallas_call(
        functools.partial(project_kernel, parts),
        out_shape=(
            jax.ShapeDtypeStruct((CORES, outs, rows), jnp.float32),
            jax.ShapeDtypeStruct((outs + 16, rows), jnp.bfloat16),
        ),
        in_specs=[smem, vmem, pl.BlockSpec(memory_space=pltpu.HBM), vmem, vmem],
        out_specs=(vmem, vmem),
        scratch_shapes=[
            pltpu.VMEM((sp, CORES, outs // CORES, LANES), jnp.bfloat16),
            pltpu.SemaphoreType.DMA((parts,)),
        ],
        compiler_params=pltpu.CompilerParams(vmem_limit_bytes=LIMIT * MEBI),
        name="project",
    )(place, stripes, everything, residual, gate)


def feed_kernel(
    place_ref, messages_ref, scales_ref, gates_ref, placed_ref, weights_ref, shares_ref, ups, downs, sems
):
    _, sp, depth, up_width = ups.shape
    whole = downs.shape[3]
    pieces = whole // LANES
    tp_size, outs, rows = gates_ref.shape
    chips = tp_size // CORES
    half = outs // PAIR
    copies, slot = ([], [], []), 0
    for kind, (first, held, count) in enumerate(
        ((half, ups, pieces), (half + 2 * pieces * depth, ups, 1), (half + pieces * depth, downs, pieces))
    ):
        for core in range(CORES):
            for j in range(count):
                lanes = (pieces if kind == 1 else j) * LANES
                copies[kind].append(
                    pltpu.make_async_copy(
                        weights_ref.at[:, core, pl.ds(first + j * depth, depth), :],
                        held.at[core, :, :, pl.ds(lanes, LANES)],
                        sems.at[slot],
                    )
                )
                slot += 1
    for group in copies:
        for copy in group:
            copy.start()
    spreads = []
    for t in range(tp_size):
        for member in range(PAIR):
            source = member * chips + t // CORES
            mean = jnp.sum(
                messages_ref[source, outs : outs + 16, :].astype(jnp.float32),
                axis=0,
                keepdims=True,
            )
            start = t % CORES * half
            spreads.append(
                messages_ref[source, start : start + half, :].astype(jnp.float32) + mean
            )
    features = tp_size * outs
    row_mean = sum(jnp.sum(part, axis=0, keepdims=True) for part in spreads) / features
    centred = [part - row_mean for part in spreads]
    spread = sum(jnp.sum(part * part, axis=0, keepdims=True) for part in centred) / features
    factor = lax.rsqrt(spread + 1e-06)
    turned = jnp.concatenate([part * factor for part in centred], axis=0).T
    normed = (turned * (1.0 + scales_ref[1:2, :]) + scales_ref[0:1, :]).astype(jnp.bfloat16)
    for copy in [*copies[0], *copies[1]]:
        copy.wait()
    active = []
    for core in range(CORES):
        for start in range(0, up_width, 2 * LANES):
            block = ups[core, :, :, start : start + 2 * LANES].reshape(sp * depth, -1)
            hidden = jnp.dot(normed, block, preferred_element_type=jnp.float32)
            active.append(jax.nn.gelu(hidden, approximate=True))
    lane = lax.broadcasted_iota(jnp.int32, (rows, LANES), 1)
    for core in range(CORES):
        tail = active[2 * core + 1]
        moved = jnp.where(lane < LANES // 2, 0.0, pltpu.roll(tail[:, LANES:], LANES // 2, 1))
        active[2 * core + 1] = jnp.concatenate([tail[:, :LANES], moved], axis=1)
    active = [part.astype(jnp.bfloat16) for part in active]
    for copy in copies[2]:
        copy.wait()
    each = sp // tp_size
    low = lax.broadcasted_iota(jnp.int32, (half, rows), 1) < rows // 2
    for t in range(tp_size):
        total = jnp.zeros((outs, rows), jnp.float32)
        for core in range(CORES):
            block = jnp.concatenate(
                [
                    downs[core, t * each : (t + 1) * each].reshape(each * depth, whole),
                    ups[core, t * each : (t + 1) * each, :, whole:].reshape(each * depth, LANES),
                ],
                axis=1,
            )
            kept = jnp.concatenate([active[2 * core], active[2 * core + 1]], axis=1)
            total = total + contract_last(block, kept)
        total = total * gates_ref[t]
        total = total + jnp.where(place_ref[0] == t // CORES, placed_ref[t % CORES], 0.0)
        top, bottom = total[:half], total[half:]
        shares_ref[0, t] = jnp.where(low, top, pltpu.roll(bottom, rows // 2, 1)).astype(
            jnp.bfloat16
        )
        shares_ref[1, t] = jnp.where(low, pltpu.roll(top, rows // 2, 1), bottom).astype(
            jnp.bfloat16
        )


def feed(place, messages, scales, gates, placed, everything, depth, units):
    tp_size, outs, rows = gates.shape
    sp = everything.shape[0]
    pieces = units // PAIR // LANES
    vmem = pl.BlockSpec(memory_space=pltpu.VMEM)
    smem = pl.BlockSpec(memory_space=pltpu.SMEM)
    return pl.pallas_call(
        feed_kernel,
        out_shape=jax.ShapeDtypeStruct((PAIR, tp_size, outs // PAIR, rows), jnp.bfloat16),
        in_specs=[smem, vmem, vmem, vmem, vmem, pl.BlockSpec(memory_space=pltpu.HBM)],
        out_specs=vmem,
        scratch_shapes=[
            pltpu.VMEM((CORES, sp, depth, (pieces + 1) * LANES), jnp.bfloat16),
            pltpu.VMEM((CORES, sp, depth, pieces * LANES), jnp.bfloat16),
            pltpu.SemaphoreType.DMA((CORES * (2 * pieces + 1),)),
        ],
        compiler_params=pltpu.CompilerParams(vmem_limit_bytes=LIMIT * MEBI),
        name="feed",
    )(place, messages, scales, gates, placed, everything)


def finish_kernel(shares_ref, out_ref):
    sources = shares_ref.shape[0]
    batches, span, _ = out_ref.shape
    for batch in range(batches):
        total = jnp.zeros(shares_ref.shape[1:], jnp.float32)
        for source in range(batch, sources, batches):
            total = total + shares_ref[source].astype(jnp.float32)
        rest = jnp.zeros((-total.shape[0] % LANES, total.shape[1]), jnp.float32)
        turned = jnp.concatenate([total, rest], axis=0).T[:, : total.shape[0]]
        both = jnp.concatenate([turned[k * span : (k + 1) * span] for k in range(PAIR)], axis=1)
        out_ref[batch] = both.astype(jnp.bfloat16)


def body(
    query_rows, key_rows, value_rows, residual, modulation, out_weight, up_weight, down_weight
):
    side, chip = lax.axis_index("member"), lax.axis_index("x")
    everything = gathered_weights(out_weight, up_weight, down_weight, side)
    tp = ("x", "core")
    tp_size = lax.axis_size(tp)
    batches, rows_block, local_width = residual.shape
    depth, units = up_weight.shape
    rows = PAIR * rows_block
    half = local_width // PAIR

    parts = residual.reshape(batches, rows_block, PAIR, half).transpose(2, 0, 1, 3)
    parts = lax.all_to_all(
        parts.reshape(PAIR * batches, rows_block, half), ("member", "core"), 0, 0, tiled=True
    )
    parts = parts.reshape(PAIR, CORES, rows_block, half).transpose(0, 2, 1, 3)
    residual_rows = parts.reshape(rows, CORES * half)
    rows_of_modulation = lax.all_gather(modulation, tp, axis=0, tiled=False)
    scales = jnp.swapaxes(rows_of_modulation[:, 1:3], 0, 1).reshape(2, -1)
    gates = jnp.broadcast_to(
        rows_of_modulation[:, 3][:, :, None], (tp_size, local_width, rows)
    )
    gate = lax.dynamic_slice_in_dim(rows_of_modulation[:, 0], chip * CORES, CORES, axis=0)
    gate = jnp.where(side == 0, gate[:, :half], gate[:, half:]).reshape(1, CORES * half)

    own = attend(query_rows, key_rows, value_rows)
    stripes = sent_to_all(own.reshape(-1, HEAD_FEATURES), ("member", "x"))
    place = jnp.stack([chip, side]).astype(jnp.int32)
    placed, message = project(place, stripes, everything, residual_rows, gate)
    messages = lax.all_gather(message, ("member", "x"), axis=0, tiled=False)
    shares = feed(place, messages, scales, gates, placed, everything, depth, units)
    shares = shares.reshape(PAIR * tp_size, half, rows)
    shares = lax.all_to_all(shares, ("member", "x", "core"), 0, 0, tiled=True)
    return pl.pallas_call(
        finish_kernel,
        out_shape=jax.ShapeDtypeStruct(residual.shape, residual.dtype),
        compiler_params=pltpu.CompilerParams(vmem_limit_bytes=8 * MEBI),
        name="finish",
    )(shares)


def solution(mesh):
    groups, tp, sp = (mesh.shape[a] for a in ("groups", "tp", "sp"))
    fine = Mesh(
        mesh.devices.reshape(groups // PAIR, PAIR, tp // CORES, CORES, sp),
        ("pairs", "member", "x", "core", "sp"),
    )
    jobs, tokens, tensor = ("pairs", "member"), ("sp", "x", "core"), ("x", "core")
    in_specs = (
        P(jobs, tokens, None),
        P(jobs, tokens, None),
        P(jobs, tokens, None),
        P(jobs, "sp", tensor),
        P(None, tensor),
        P(tensor, "sp"),
        P("sp", tensor),
        P("sp", tensor),
    )
    out_specs = P(jobs, "sp", tensor)
    return jax.shard_map(body, mesh=fine, in_specs=in_specs, out_specs=out_specs, check_vma=False)
```

```python
import functools
import math

import jax
import jax.numpy as jnp
from jax import lax
from jax.experimental import pallas as pl
from jax.experimental.pallas import tpu as pltpu
from jax.sharding import Mesh, PartitionSpec as P

HEAD_FEATURES = 128
LANES = 128
CORES = 2
PAIR = 2
MEBI = 1 << 20
LIMIT = 48
MEAN_PARTS = 3


def contract_last(left, right):
    return lax.dot_general(
        left, right, (((1,), (1,)), ((), ())), preferred_element_type=jnp.float32
    )


def sent_to_all(array, axis):
    copies = jnp.broadcast_to(array, (lax.axis_size(axis), *array.shape))
    return lax.all_to_all(copies, axis, split_axis=0, concat_axis=0, tiled=True)


def gathered_weights(out_weight, up_weight, down_weight, side):
    depth, units = up_weight.shape
    outs = out_weight.shape[0]

    def half(array, dim):
        size = array.shape[dim] // PAIR
        parts = [lax.slice_in_dim(array, k * size, (k + 1) * size, axis=dim) for k in range(PAIR)]
        return jnp.where(side == 0, parts[0], parts[1])

    up_half, down_half = half(up_weight, 1), half(down_weight, 1)
    whole = units // PAIR // LANES * LANES
    pieces = [half(out_weight, 0)]
    for matrix in (up_half, down_half):
        for start in range(0, whole, LANES):
            pieces.append(matrix[:, start : start + LANES])
    pieces.append(jnp.concatenate([up_half[:, whole:], down_half[:, whole:]], axis=1))
    packed = jnp.concatenate(pieces, axis=0)
    everything = lax.all_gather(packed, ("sp", "core"), axis=0, tiled=False)
    return everything.reshape(lax.axis_size("sp"), CORES, *packed.shape)


def attend(query_part, key_part, value_part):
    sp = lax.axis_size("sp")
    batches, rows, width = query_part.shape
    heads = width // HEAD_FEATURES
    both = jnp.stack([query_part, key_part, value_part], axis=1)
    both = both.reshape(batches, 3, rows, heads, HEAD_FEATURES).transpose(0, 3, 1, 2, 4)
    swapped = lax.all_to_all(both, "core", split_axis=0, concat_axis=0, tiled=True)
    to_heads = jnp.swapaxes(swapped, 0, 1).reshape(sp, CORES * 3 * rows, HEAD_FEATURES)
    here = lax.all_to_all(to_heads, "sp", split_axis=0, concat_axis=0, tiled=True)
    here = here.reshape(sp, CORES, 3, rows, HEAD_FEATURES)
    count = sp * CORES * rows
    queries = here[:, :, 0].reshape(count, HEAD_FEATURES)
    own = here[:, :, 1:].transpose(2, 0, 1, 3, 4).reshape(2, count, HEAD_FEATURES)
    gathered = sent_to_all(own, "x")
    keys = gathered[:, 0].reshape(-1, HEAD_FEATURES)
    values = gathered[:, 1].reshape(-1, HEAD_FEATURES)
    scores = contract_last(queries, keys) * (1.0 / math.sqrt(HEAD_FEATURES))
    exponent = jnp.exp(scores - jnp.max(scores, axis=-1, keepdims=True))
    row_total = jnp.sum(exponent, axis=-1, keepdims=True)
    weighted = jnp.dot(
        exponent.astype(jnp.bfloat16), values, preferred_element_type=jnp.float32
    )
    attended = (weighted / row_total).astype(jnp.bfloat16)
    back = attended.reshape(sp, CORES * rows, HEAD_FEATURES)
    return lax.all_to_all(back, "sp", split_axis=0, concat_axis=0, tiled=True)


def project_kernel(
    parts, place_ref, stripes_ref, weights_ref, residual_ref, gate_ref, placed_ref, message_ref, held, sems
):
    heads, _, half, _ = held.shape
    width = CORES * half
    each = heads // parts
    copies = [
        pltpu.make_async_copy(
            weights_ref.at[pl.ds(k * each, each), :, pl.ds(0, half), :],
            held.at[pl.ds(k * each, each)],
            sems.at[k],
        )
        for k in range(parts)
    ]
    for copy in copies:
        copy.start()
    sources = stripes_ref.shape[0]
    rows = residual_ref.shape[0]
    span = rows // sources
    residual = residual_ref[...].astype(jnp.float32)
    placed_ref[...] = jnp.zeros(placed_ref.shape, jnp.float32)
    total = jnp.zeros(residual.shape, jnp.float32)
    for k in range(parts):
        copies[k].wait()
        for h in range(k * each, (k + 1) * each, 2):
            left, right = (
                jnp.concatenate(pair, axis=1)
                for pair in (
                    [
                        stripes_ref[:, i * span : (i + 1) * span, :].reshape(-1, LANES)
                        for i in (h, h + 1)
                    ],
                    [held[i].reshape(width, LANES) for i in (h, h + 1)],
                )
            )
            total = total + contract_last(left, right)
    mixed = residual + gate_ref[...] * total
    mean = jnp.mean(mixed, axis=1, keepdims=True)
    left, told, columns = mean, jnp.zeros_like(mean), []
    for _ in range(MEAN_PARTS):
        columns.append(left.astype(jnp.bfloat16).astype(jnp.float32))
        told = told + columns[-1]
        left = mean - told
    lane = lax.broadcasted_iota(jnp.int32, (rows, -width % LANES), 1)
    rest = jnp.zeros(lane.shape, jnp.float32)
    for k, column in enumerate(columns):
        rest = jnp.where(lane == k, column, rest)
    rest = jnp.where(lane == 16, told, rest)
    turned = jnp.concatenate([mixed, rest], axis=1).T
    deviation = (turned[0:width] - turned[width + 16 : width + 17]).astype(jnp.bfloat16)
    means = turned[width : width + 16].astype(jnp.bfloat16)
    for k in range(message_ref.shape[0]):
        message_ref[k, 0:width, :] = deviation
        message_ref[k, width : width + 16, :] = means
    at = pl.multiple_of(place_ref[1] * half, half)
    for core in range(CORES):
        placed_ref[core, pl.ds(at, half), :] = turned[core * half : (core + 1) * half]


def project(place, stripes, everything, residual, gate):
    rows, outs = residual.shape
    sp = everything.shape[0]
    parts = 8
    vmem = pl.BlockSpec(memory_space=pltpu.VMEM)
    smem = pl.BlockSpec(memory_space=pltpu.SMEM)
    return pl.pallas_call(
        functools.partial(project_kernel, parts),
        out_shape=(
            jax.ShapeDtypeStruct((CORES, outs, rows), jnp.float32),
            jax.ShapeDtypeStruct((stripes.shape[0], outs + 16, rows), jnp.bfloat16),
        ),
        in_specs=[smem, vmem, pl.BlockSpec(memory_space=pltpu.HBM), vmem, vmem],
        out_specs=(vmem, vmem),
        scratch_shapes=[
            pltpu.VMEM((sp, CORES, outs // CORES, LANES), jnp.bfloat16),
            pltpu.SemaphoreType.DMA((parts,)),
        ],
        compiler_params=pltpu.CompilerParams(vmem_limit_bytes=LIMIT * MEBI),
        name="project",
    )(place, stripes, everything, residual, gate)


def feed_kernel(
    place_ref, messages_ref, scales_ref, gates_ref, placed_ref, weights_ref, shares_ref, ups, downs, sems
):
    _, sp, depth, up_width = ups.shape
    whole = downs.shape[3]
    pieces = whole // LANES
    tp_size, outs, rows = gates_ref.shape
    chips = tp_size // CORES
    half = outs // PAIR
    copies, slot = ([], [], []), 0
    for kind, (first, held, count) in enumerate(
        ((half, ups, pieces), (half + 2 * pieces * depth, ups, 1), (half + pieces * depth, downs, pieces))
    ):
        for core in range(CORES):
            for j in range(count):
                lanes = (pieces if kind == 1 else j) * LANES
                copies[kind].append(
                    pltpu.make_async_copy(
                        weights_ref.at[:, core, pl.ds(first + j * depth, depth), :],
                        held.at[core, :, :, pl.ds(lanes, LANES)],
                        sems.at[slot],
                    )
                )
                slot += 1
    for group in copies:
        for copy in group:
            copy.start()
    spreads = []
    for t in range(tp_size):
        for member in range(PAIR):
            source = member * chips + t // CORES
            mean = jnp.sum(
                messages_ref[source, outs : outs + 16, :].astype(jnp.float32),
                axis=0,
                keepdims=True,
            )
            start = t % CORES * half
            spreads.append(
                messages_ref[source, start : start + half, :].astype(jnp.float32) + mean
            )
    features = tp_size * outs
    row_mean = sum(jnp.sum(part, axis=0, keepdims=True) for part in spreads) / features
    centred = [part - row_mean for part in spreads]
    spread = sum(jnp.sum(part * part, axis=0, keepdims=True) for part in centred) / features
    factor = lax.rsqrt(spread + 1e-06)
    turned = jnp.concatenate([part * factor for part in centred], axis=0).T
    normed = (turned * (1.0 + scales_ref[1:2, :]) + scales_ref[0:1, :]).astype(jnp.bfloat16)
    for copy in [*copies[0], *copies[1]]:
        copy.wait()
    active = []
    for core in range(CORES):
        for start in range(0, up_width, 2 * LANES):
            block = ups[core, :, :, start : start + 2 * LANES].reshape(sp * depth, -1)
            hidden = jnp.dot(normed, block, preferred_element_type=jnp.float32)
            active.append(jax.nn.gelu(hidden, approximate=True))
    lane = lax.broadcasted_iota(jnp.int32, (rows, LANES), 1)
    for core in range(CORES):
        tail = active[2 * core + 1]
        moved = jnp.where(lane < LANES // 2, 0.0, pltpu.roll(tail[:, LANES:], LANES // 2, 1))
        active[2 * core + 1] = jnp.concatenate([tail[:, :LANES], moved], axis=1)
    active = [part.astype(jnp.bfloat16) for part in active]
    for copy in copies[2]:
        copy.wait()
    each = sp // tp_size
    low = lax.broadcasted_iota(jnp.int32, (half, rows), 1) < rows // 2
    for t in range(tp_size):
        total = jnp.zeros((outs, rows), jnp.float32)
        for core in range(CORES):
            block = jnp.concatenate(
                [
                    downs[core, t * each : (t + 1) * each].reshape(each * depth, whole),
                    ups[core, t * each : (t + 1) * each, :, whole:].reshape(each * depth, LANES),
                ],
                axis=1,
            )
            kept = jnp.concatenate([active[2 * core], active[2 * core + 1]], axis=1)
            total = total + contract_last(block, kept)
        total = total * gates_ref[t]
        total = total + jnp.where(place_ref[0] == t // CORES, placed_ref[t % CORES], 0.0)
        top, bottom = total[:half], total[half:]
        shares_ref[0, t] = jnp.where(low, top, pltpu.roll(bottom, rows // 2, 1)).astype(
            jnp.bfloat16
        )
        shares_ref[1, t] = jnp.where(low, pltpu.roll(top, rows // 2, 1), bottom).astype(
            jnp.bfloat16
        )


def feed(place, messages, scales, gates, placed, everything, depth, units):
    tp_size, outs, rows = gates.shape
    sp = everything.shape[0]
    pieces = units // PAIR // LANES
    vmem = pl.BlockSpec(memory_space=pltpu.VMEM)
    smem = pl.BlockSpec(memory_space=pltpu.SMEM)
    return pl.pallas_call(
        feed_kernel,
        out_shape=jax.ShapeDtypeStruct((PAIR, tp_size, outs // PAIR, rows), jnp.bfloat16),
        in_specs=[smem, vmem, vmem, vmem, vmem, pl.BlockSpec(memory_space=pltpu.HBM)],
        out_specs=vmem,
        scratch_shapes=[
            pltpu.VMEM((CORES, sp, depth, (pieces + 1) * LANES), jnp.bfloat16),
            pltpu.VMEM((CORES, sp, depth, pieces * LANES), jnp.bfloat16),
            pltpu.SemaphoreType.DMA((CORES * (2 * pieces + 1),)),
        ],
        compiler_params=pltpu.CompilerParams(vmem_limit_bytes=LIMIT * MEBI),
        name="feed",
    )(place, messages, scales, gates, placed, everything)


def finish_kernel(shares_ref, out_ref):
    sources = shares_ref.shape[0]
    batches, span, _ = out_ref.shape
    for batch in range(batches):
        total = jnp.zeros(shares_ref.shape[1:], jnp.float32)
        for source in range(batch, sources, batches):
            total = total + shares_ref[source].astype(jnp.float32)
        rest = jnp.zeros((-total.shape[0] % LANES, total.shape[1]), jnp.float32)
        turned = jnp.concatenate([total, rest], axis=0).T[:, : total.shape[0]]
        both = jnp.concatenate([turned[k * span : (k + 1) * span] for k in range(PAIR)], axis=1)
        out_ref[batch] = both.astype(jnp.bfloat16)


def body(
    query_rows, key_rows, value_rows, residual, modulation, out_weight, up_weight, down_weight
):
    side, chip = lax.axis_index("member"), lax.axis_index("x")
    everything = gathered_weights(out_weight, up_weight, down_weight, side)
    tp = ("x", "core")
    tp_size = lax.axis_size(tp)
    batches, rows_block, local_width = residual.shape
    depth, units = up_weight.shape
    rows = PAIR * rows_block
    half = local_width // PAIR

    parts = residual.reshape(batches, rows_block, PAIR, half).transpose(2, 0, 1, 3)
    parts = lax.all_to_all(
        parts.reshape(PAIR * batches, rows_block, half), ("member", "core"), 0, 0, tiled=True
    )
    parts = parts.reshape(PAIR, CORES, rows_block, half).transpose(0, 2, 1, 3)
    residual_rows = parts.reshape(rows, CORES * half)
    rows_of_modulation = lax.all_gather(modulation, tp, axis=0, tiled=False)
    scales = jnp.swapaxes(rows_of_modulation[:, 1:3], 0, 1).reshape(2, -1)
    gates = jnp.broadcast_to(
        rows_of_modulation[:, 3][:, :, None], (tp_size, local_width, rows)
    )
    gate = lax.dynamic_slice_in_dim(rows_of_modulation[:, 0], chip * CORES, CORES, axis=0)
    gate = jnp.where(side == 0, gate[:, :half], gate[:, half:]).reshape(1, CORES * half)

    own = attend(query_rows, key_rows, value_rows)
    stripes = sent_to_all(own.reshape(-1, HEAD_FEATURES), ("member", "x"))
    place = jnp.stack([chip, side]).astype(jnp.int32)
    stripes, gates = lax.optimization_barrier((stripes, gates))
    placed, messages = project(place, stripes, everything, residual_rows, gate)
    messages = lax.all_to_all(messages, ("member", "x"), 0, 0, tiled=True)
    shares = feed(place, messages, scales, gates, placed, everything, depth, units)
    shares = shares.reshape(PAIR * tp_size, half, rows)
    shares = lax.all_to_all(shares, ("member", "x", "core"), 0, 0, tiled=True)
    return pl.pallas_call(
        finish_kernel,
        out_shape=jax.ShapeDtypeStruct(residual.shape, residual.dtype),
        compiler_params=pltpu.CompilerParams(vmem_limit_bytes=8 * MEBI),
        name="finish",
    )(shares)


def solution(mesh):
    groups, tp, sp = (mesh.shape[a] for a in ("groups", "tp", "sp"))
    fine = Mesh(
        mesh.devices.reshape(groups // PAIR, PAIR, tp // CORES, CORES, sp),
        ("pairs", "member", "x", "core", "sp"),
    )
    jobs, tokens, tensor = ("pairs", "member"), ("sp", "x", "core"), ("x", "core")
    in_specs = (
        P(jobs, tokens, None),
        P(jobs, tokens, None),
        P(jobs, tokens, None),
        P(jobs, "sp", tensor),
        P(None, tensor),
        P(tensor, "sp"),
        P("sp", tensor),
        P("sp", tensor),
    )
    out_specs = P(jobs, "sp", tensor)
    return jax.shard_map(body, mesh=fine, in_specs=in_specs, out_specs=out_specs, check_vma=False)
```

```python
import functools
import math

import jax
import jax.numpy as jnp
from jax import lax
from jax.experimental import pallas as pl
from jax.experimental.pallas import tpu as pltpu
from jax.sharding import Mesh, PartitionSpec as P

HEAD_FEATURES = 128
LANES = 128
CORES = 2
PAIR = 2
MEBI = 1 << 20
LIMIT = 48
MEAN_PARTS = 3


def contract_last(left, right):
    return lax.dot_general(
        left, right, (((1,), (1,)), ((), ())), preferred_element_type=jnp.float32
    )


def sent_to_all(array, axis):
    copies = jnp.broadcast_to(array, (lax.axis_size(axis), *array.shape))
    return lax.all_to_all(copies, axis, split_axis=0, concat_axis=0, tiled=True)


def gathered_weights(out_weight, up_weight, down_weight, side):
    depth, units = up_weight.shape
    outs = out_weight.shape[0]

    def half(array, dim):
        size = array.shape[dim] // PAIR
        parts = [lax.slice_in_dim(array, k * size, (k + 1) * size, axis=dim) for k in range(PAIR)]
        return jnp.where(side == 0, parts[0], parts[1])

    up_half, down_half = half(up_weight, 1), half(down_weight, 1)
    whole = units // PAIR // LANES * LANES
    pieces = [half(out_weight, 0)]
    for matrix in (up_half, down_half):
        for start in range(0, whole, LANES):
            pieces.append(matrix[:, start : start + LANES])
    pieces.append(jnp.concatenate([up_half[:, whole:], down_half[:, whole:]], axis=1))
    packed = jnp.concatenate(pieces, axis=0)
    everything = lax.all_gather(packed, ("sp", "core"), axis=0, tiled=False)
    return everything.reshape(lax.axis_size("sp"), CORES, *packed.shape)


def attend(query_part, key_part, value_part):
    sp = lax.axis_size("sp")
    batches, rows, width = query_part.shape
    heads = width // HEAD_FEATURES
    both = jnp.stack([query_part, key_part, value_part], axis=1)
    both = both.reshape(batches, 3, rows, heads, HEAD_FEATURES).transpose(0, 3, 1, 2, 4)
    swapped = lax.all_to_all(both, "core", split_axis=0, concat_axis=0, tiled=True)
    to_heads = jnp.swapaxes(swapped, 0, 1).reshape(sp, CORES * 3 * rows, HEAD_FEATURES)
    here = lax.all_to_all(to_heads, "sp", split_axis=0, concat_axis=0, tiled=True)
    here = here.reshape(sp, CORES, 3, rows, HEAD_FEATURES)
    count = sp * CORES * rows
    queries = here[:, :, 0].reshape(count, HEAD_FEATURES)
    own = here[:, :, 1:].transpose(2, 0, 1, 3, 4).reshape(2, count, HEAD_FEATURES)
    gathered = sent_to_all(own, "x")
    keys = gathered[:, 0].reshape(-1, HEAD_FEATURES)
    values = gathered[:, 1].reshape(-1, HEAD_FEATURES)
    scores = contract_last(queries, keys) * (1.0 / math.sqrt(HEAD_FEATURES))
    exponent = jnp.exp(scores - jnp.max(scores, axis=-1, keepdims=True))
    row_total = jnp.sum(exponent, axis=-1, keepdims=True)
    weighted = jnp.dot(
        exponent.astype(jnp.bfloat16), values, preferred_element_type=jnp.float32
    )
    attended = (weighted / row_total).astype(jnp.bfloat16)
    back = attended.reshape(sp, CORES * rows, HEAD_FEATURES)
    return lax.all_to_all(back, "sp", split_axis=0, concat_axis=0, tiled=True)


def project_kernel(
    parts, place_ref, stripes_ref, weights_ref, residual_ref, gate_ref, placed_ref, message_ref, held, sems
):
    heads, _, half, _ = held.shape
    width = CORES * half
    each = heads // parts
    copies = [
        pltpu.make_async_copy(
            weights_ref.at[pl.ds(k * each, each), :, pl.ds(0, half), :],
            held.at[pl.ds(k * each, each)],
            sems.at[k],
        )
        for k in range(parts)
    ]
    for copy in copies:
        copy.start()
    sources = stripes_ref.shape[0]
    rows = residual_ref.shape[0]
    span = rows // sources
    residual = residual_ref[...].astype(jnp.float32)
    placed_ref[...] = jnp.zeros(placed_ref.shape, jnp.float32)
    total = jnp.zeros(residual.shape, jnp.float32)
    for k in range(parts):
        copies[k].wait()
        for h in range(k * each, (k + 1) * each, 2):
            left, right = (
                jnp.concatenate(pair, axis=1)
                for pair in (
                    [
                        stripes_ref[:, i * span : (i + 1) * span, :].reshape(-1, LANES)
                        for i in (h, h + 1)
                    ],
                    [held[i].reshape(width, LANES) for i in (h, h + 1)],
                )
            )
            total = total + contract_last(left, right)
    mixed = residual + gate_ref[...] * total
    mean = jnp.mean(mixed, axis=1, keepdims=True)
    left, told, columns = mean, jnp.zeros_like(mean), []
    for _ in range(MEAN_PARTS):
        columns.append(left.astype(jnp.bfloat16).astype(jnp.float32))
        told = told + columns[-1]
        left = mean - told
    lane = lax.broadcasted_iota(jnp.int32, (rows, -width % LANES), 1)
    rest = jnp.zeros(lane.shape, jnp.float32)
    for k, column in enumerate(columns):
        rest = jnp.where(lane == k, column, rest)
    rest = jnp.where(lane == 16, told, rest)
    turned = jnp.concatenate([mixed, rest], axis=1).T
    deviation = (turned[0:width] - turned[width + 16 : width + 17]).astype(jnp.bfloat16)
    means = turned[width : width + 16].astype(jnp.bfloat16)
    for k in range(message_ref.shape[0]):
        message_ref[k, 0:width, :] = deviation
        message_ref[k, width : width + 16, :] = means
    at = pl.multiple_of(place_ref[1] * half, half)
    for core in range(CORES):
        placed_ref[core, pl.ds(at, half), :] = turned[core * half : (core + 1) * half]


def project(place, stripes, everything, residual, gate):
    rows, outs = residual.shape
    sp = everything.shape[0]
    parts = 8
    vmem = pl.BlockSpec(memory_space=pltpu.VMEM)
    smem = pl.BlockSpec(memory_space=pltpu.SMEM)
    return pl.pallas_call(
        functools.partial(project_kernel, parts),
        out_shape=(
            jax.ShapeDtypeStruct((CORES, outs, rows), jnp.float32),
            jax.ShapeDtypeStruct((stripes.shape[0], outs + 16, rows), jnp.bfloat16),
        ),
        in_specs=[smem, vmem, pl.BlockSpec(memory_space=pltpu.HBM), vmem, vmem],
        out_specs=(vmem, vmem),
        scratch_shapes=[
            pltpu.VMEM((sp, CORES, outs // CORES, LANES), jnp.bfloat16),
            pltpu.SemaphoreType.DMA((parts,)),
        ],
        compiler_params=pltpu.CompilerParams(vmem_limit_bytes=LIMIT * MEBI),
        name="project",
    )(place, stripes, everything, residual, gate)


def feed_kernel(
    place_ref, messages_ref, scales_ref, gates_ref, placed_ref, weights_ref, shares_ref, ups, downs, sems
):
    _, sp, depth, up_width = ups.shape
    whole = downs.shape[3]
    pieces = whole // LANES
    tp_size, outs, rows = gates_ref.shape
    chips = tp_size // CORES
    half = outs // PAIR
    copies, slot = ([], [], []), 0
    for kind, (first, held, count) in enumerate(
        ((half, ups, pieces), (half + 2 * pieces * depth, ups, 1), (half + pieces * depth, downs, pieces))
    ):
        for core in range(CORES):
            for j in range(count):
                lanes = (pieces if kind == 1 else j) * LANES
                copies[kind].append(
                    pltpu.make_async_copy(
                        weights_ref.at[:, core, pl.ds(first + j * depth, depth), :],
                        held.at[core, :, :, pl.ds(lanes, LANES)],
                        sems.at[slot],
                    )
                )
                slot += 1
    ordered = []
    for core in range(CORES):
        ordered += [*copies[0][core * pieces : (core + 1) * pieces], copies[1][core]]
    for copy in [*ordered, *copies[2]]:
        copy.start()
    spreads = []
    for t in range(tp_size):
        for member in range(PAIR):
            source = member * chips + t // CORES
            mean = jnp.sum(
                messages_ref[source, outs : outs + 16, :].astype(jnp.float32),
                axis=0,
                keepdims=True,
            )
            start = t % CORES * half
            spreads.append(
                messages_ref[source, start : start + half, :].astype(jnp.float32) + mean
            )
    features = tp_size * outs
    row_mean = sum(jnp.sum(part, axis=0, keepdims=True) for part in spreads) / features
    centred = [part - row_mean for part in spreads]
    spread = sum(jnp.sum(part * part, axis=0, keepdims=True) for part in centred) / features
    factor = lax.rsqrt(spread + 1e-06)
    turned = jnp.concatenate([part * factor for part in centred], axis=0).T
    normed = (turned * (1.0 + scales_ref[1:2, :]) + scales_ref[0:1, :]).astype(jnp.bfloat16)
    active = []
    for core in range(CORES):
        for start in range(0, up_width, 2 * LANES):
            first = core * (pieces + 1) + start // LANES
            for copy in ordered[first : first + 2]:
                copy.wait()
            block = ups[core, :, :, start : start + 2 * LANES].reshape(sp * depth, -1)
            hidden = jnp.dot(normed, block, preferred_element_type=jnp.float32)
            active.append(jax.nn.gelu(hidden, approximate=True))
    lane = lax.broadcasted_iota(jnp.int32, (rows, LANES), 1)
    for core in range(CORES):
        tail = active[2 * core + 1]
        moved = jnp.where(lane < LANES // 2, 0.0, pltpu.roll(tail[:, LANES:], LANES // 2, 1))
        active[2 * core + 1] = jnp.concatenate([tail[:, :LANES], moved], axis=1)
    active = [part.astype(jnp.bfloat16) for part in active]
    for copy in copies[2]:
        copy.wait()
    each = sp // tp_size
    low = lax.broadcasted_iota(jnp.int32, (half, rows), 1) < rows // 2
    for t in range(tp_size):
        total = jnp.zeros((outs, rows), jnp.float32)
        for core in range(CORES):
            block = jnp.concatenate(
                [
                    downs[core, t * each : (t + 1) * each].reshape(each * depth, whole),
                    ups[core, t * each : (t + 1) * each, :, whole:].reshape(each * depth, LANES),
                ],
                axis=1,
            )
            kept = jnp.concatenate([active[2 * core], active[2 * core + 1]], axis=1)
            total = total + contract_last(block, kept)
        total = total * gates_ref[t]
        total = total + jnp.where(place_ref[0] == t // CORES, placed_ref[t % CORES], 0.0)
        top, bottom = total[:half], total[half:]
        shares_ref[0, t] = jnp.where(low, top, pltpu.roll(bottom, rows // 2, 1)).astype(
            jnp.bfloat16
        )
        shares_ref[1, t] = jnp.where(low, pltpu.roll(top, rows // 2, 1), bottom).astype(
            jnp.bfloat16
        )


def feed(place, messages, scales, gates, placed, everything, depth, units):
    tp_size, outs, rows = gates.shape
    sp = everything.shape[0]
    pieces = units // PAIR // LANES
    vmem = pl.BlockSpec(memory_space=pltpu.VMEM)
    smem = pl.BlockSpec(memory_space=pltpu.SMEM)
    return pl.pallas_call(
        feed_kernel,
        out_shape=jax.ShapeDtypeStruct((PAIR, tp_size, outs // PAIR, rows), jnp.bfloat16),
        in_specs=[smem, vmem, vmem, vmem, vmem, pl.BlockSpec(memory_space=pltpu.HBM)],
        out_specs=vmem,
        scratch_shapes=[
            pltpu.VMEM((CORES, sp, depth, (pieces + 1) * LANES), jnp.bfloat16),
            pltpu.VMEM((CORES, sp, depth, pieces * LANES), jnp.bfloat16),
            pltpu.SemaphoreType.DMA((CORES * (2 * pieces + 1),)),
        ],
        compiler_params=pltpu.CompilerParams(vmem_limit_bytes=LIMIT * MEBI),
        name="feed",
    )(place, messages, scales, gates, placed, everything)


def finish_kernel(shares_ref, out_ref):
    sources = shares_ref.shape[0]
    batches, span, _ = out_ref.shape
    for batch in range(batches):
        total = jnp.zeros(shares_ref.shape[1:], jnp.float32)
        for source in range(batch, sources, batches):
            total = total + shares_ref[source].astype(jnp.float32)
        rest = jnp.zeros((-total.shape[0] % LANES, total.shape[1]), jnp.float32)
        turned = jnp.concatenate([total, rest], axis=0).T[:, : total.shape[0]]
        both = jnp.concatenate([turned[k * span : (k + 1) * span] for k in range(PAIR)], axis=1)
        out_ref[batch] = both.astype(jnp.bfloat16)


def body(
    query_rows, key_rows, value_rows, residual, modulation, out_weight, up_weight, down_weight
):
    side, chip = lax.axis_index("member"), lax.axis_index("x")
    everything = gathered_weights(out_weight, up_weight, down_weight, side)
    tp = ("x", "core")
    tp_size = lax.axis_size(tp)
    batches, rows_block, local_width = residual.shape
    depth, units = up_weight.shape
    rows = PAIR * rows_block
    half = local_width // PAIR

    parts = residual.reshape(batches, rows_block, PAIR, half).transpose(2, 0, 1, 3)
    parts = lax.all_to_all(
        parts.reshape(PAIR * batches, rows_block, half), ("member", "core"), 0, 0, tiled=True
    )
    parts = parts.reshape(PAIR, CORES, rows_block, half).transpose(0, 2, 1, 3)
    residual_rows = parts.reshape(rows, CORES * half)
    rows_of_modulation = lax.all_gather(modulation, tp, axis=0, tiled=False)
    scales = jnp.swapaxes(rows_of_modulation[:, 1:3], 0, 1).reshape(2, -1)
    gates = jnp.broadcast_to(
        rows_of_modulation[:, 3][:, :, None], (tp_size, local_width, rows)
    )
    gate = lax.dynamic_slice_in_dim(rows_of_modulation[:, 0], chip * CORES, CORES, axis=0)
    gate = jnp.where(side == 0, gate[:, :half], gate[:, half:]).reshape(1, CORES * half)

    own = attend(query_rows, key_rows, value_rows)
    stripes = sent_to_all(own.reshape(-1, HEAD_FEATURES), ("member", "x"))
    place = jnp.stack([chip, side]).astype(jnp.int32)
    stripes, gates = lax.optimization_barrier((stripes, gates))
    placed, messages = project(place, stripes, everything, residual_rows, gate)
    messages = lax.all_to_all(messages, ("member", "x"), 0, 0, tiled=True)
    shares = feed(place, messages, scales, gates, placed, everything, depth, units)
    shares = shares.reshape(PAIR * tp_size, half, rows)
    shares = lax.all_to_all(shares, ("member", "x", "core"), 0, 0, tiled=True)
    return pl.pallas_call(
        finish_kernel,
        out_shape=jax.ShapeDtypeStruct(residual.shape, residual.dtype),
        compiler_params=pltpu.CompilerParams(vmem_limit_bytes=8 * MEBI),
        name="finish",
    )(shares)


def solution(mesh):
    groups, tp, sp = (mesh.shape[a] for a in ("groups", "tp", "sp"))
    fine = Mesh(
        mesh.devices.reshape(groups // PAIR, PAIR, tp // CORES, CORES, sp),
        ("pairs", "member", "x", "core", "sp"),
    )
    jobs, tokens, tensor = ("pairs", "member"), ("sp", "x", "core"), ("x", "core")
    in_specs = (
        P(jobs, tokens, None),
        P(jobs, tokens, None),
        P(jobs, tokens, None),
        P(jobs, "sp", tensor),
        P(None, tensor),
        P(tensor, "sp"),
        P("sp", tensor),
        P("sp", tensor),
    )
    out_specs = P(jobs, "sp", tensor)
    return jax.shard_map(body, mesh=fine, in_specs=in_specs, out_specs=out_specs, check_vma=False)
```

```python
import functools
import math

import jax
import jax.numpy as jnp
from jax import lax
from jax.experimental import pallas as pl
from jax.experimental.pallas import tpu as pltpu
from jax.sharding import Mesh, PartitionSpec as P

HEAD_FEATURES = 128
LANES = 128
CORES = 2
PAIR = 2
MEBI = 1 << 20
LIMIT = 48
MEAN_PARTS = 3


def contract_last(left, right):
    return lax.dot_general(
        left, right, (((1,), (1,)), ((), ())), preferred_element_type=jnp.float32
    )


def sent_to_all(array, axis):
    copies = jnp.broadcast_to(array, (lax.axis_size(axis), *array.shape))
    return lax.all_to_all(copies, axis, split_axis=0, concat_axis=0, tiled=True)


def gathered_weights(out_weight, up_weight, down_weight, side):
    depth, units = up_weight.shape
    outs = out_weight.shape[0]

    def half(array, dim):
        size = array.shape[dim] // PAIR
        parts = [lax.slice_in_dim(array, k * size, (k + 1) * size, axis=dim) for k in range(PAIR)]
        return jnp.where(side == 0, parts[0], parts[1])

    up_half, down_half = half(up_weight, 1), half(down_weight, 1)
    whole = units // PAIR // LANES * LANES
    pieces = [half(out_weight, 0)]
    for matrix in (up_half, down_half):
        for start in range(0, whole, LANES):
            pieces.append(matrix[:, start : start + LANES])
    pieces.append(jnp.concatenate([up_half[:, whole:], down_half[:, whole:]], axis=1))
    packed = jnp.concatenate(pieces, axis=0)
    everything = lax.all_gather(packed, ("sp", "core"), axis=0, tiled=False)
    return everything.reshape(lax.axis_size("sp"), CORES, *packed.shape)


def attend(query_part, key_part, value_part):
    sp = lax.axis_size("sp")
    batches, rows, width = query_part.shape
    heads = width // HEAD_FEATURES
    both = jnp.stack([query_part, key_part, value_part], axis=1)
    both = both.reshape(batches, 3, rows, heads, HEAD_FEATURES).transpose(0, 3, 1, 2, 4)
    swapped = lax.all_to_all(both, "core", split_axis=0, concat_axis=0, tiled=True)
    to_heads = jnp.swapaxes(swapped, 0, 1).reshape(sp, CORES * 3 * rows, HEAD_FEATURES)
    here = lax.all_to_all(to_heads, "sp", split_axis=0, concat_axis=0, tiled=True)
    here = here.reshape(sp, CORES, 3, rows, HEAD_FEATURES)
    count = sp * CORES * rows
    queries = here[:, :, 0].reshape(count, HEAD_FEATURES)
    own = here[:, :, 1:].transpose(2, 0, 1, 3, 4).reshape(2, count, HEAD_FEATURES)
    gathered = sent_to_all(own, "x")
    keys = gathered[:, 0].reshape(-1, HEAD_FEATURES)
    values = gathered[:, 1].reshape(-1, HEAD_FEATURES)
    scores = contract_last(queries, keys) * (1.0 / math.sqrt(HEAD_FEATURES))
    exponent = jnp.exp(scores - jnp.max(scores, axis=-1, keepdims=True))
    row_total = jnp.sum(exponent, axis=-1, keepdims=True)
    weighted = jnp.dot(
        exponent.astype(jnp.bfloat16), values, preferred_element_type=jnp.float32
    )
    attended = (weighted / row_total).astype(jnp.bfloat16)
    back = attended.reshape(sp, CORES * rows, HEAD_FEATURES)
    return lax.all_to_all(back, "sp", split_axis=0, concat_axis=0, tiled=True)


def project_kernel(
    parts, place_ref, stripes_ref, weights_ref, residual_ref, gate_ref, placed_ref, message_ref, held, sems
):
    heads, _, half, _ = held.shape
    width = CORES * half
    each = heads // parts
    copies = [
        pltpu.make_async_copy(
            weights_ref.at[pl.ds(k * each, each), :, pl.ds(0, half), :],
            held.at[pl.ds(k * each, each)],
            sems.at[k],
        )
        for k in range(parts)
    ]
    for copy in copies:
        copy.start()
    sources = stripes_ref.shape[0]
    rows = residual_ref.shape[0]
    span = rows // sources
    residual = residual_ref[...].astype(jnp.float32)
    placed_ref[...] = jnp.zeros(placed_ref.shape, jnp.float32)
    total = jnp.zeros(residual.shape, jnp.float32)
    for k in range(parts):
        copies[k].wait()
        for h in range(k * each, (k + 1) * each, 2):
            left, right = (
                jnp.concatenate(pair, axis=1)
                for pair in (
                    [
                        stripes_ref[:, i * span : (i + 1) * span, :].reshape(-1, LANES)
                        for i in (h, h + 1)
                    ],
                    [held[i].reshape(width, LANES) for i in (h, h + 1)],
                )
            )
            total = total + contract_last(left, right)
    mixed = residual + gate_ref[...] * total
    mean = jnp.mean(mixed, axis=1, keepdims=True)
    left, told, columns = mean, jnp.zeros_like(mean), []
    for _ in range(MEAN_PARTS):
        columns.append(left.astype(jnp.bfloat16).astype(jnp.float32))
        told = told + columns[-1]
        left = mean - told
    lane = lax.broadcasted_iota(jnp.int32, (rows, -width % LANES), 1)
    rest = jnp.zeros(lane.shape, jnp.float32)
    for k, column in enumerate(columns):
        rest = jnp.where(lane == k, column, rest)
    rest = jnp.where(lane == 16, told, rest)
    turned = jnp.concatenate([mixed, rest], axis=1).T
    deviation = (turned[0:width] - turned[width + 16 : width + 17]).astype(jnp.bfloat16)
    means = turned[width : width + 16].astype(jnp.bfloat16)
    for k in range(message_ref.shape[0]):
        message_ref[k, 0:width, :] = deviation
        message_ref[k, width : width + 16, :] = means
    at = pl.multiple_of(place_ref[1] * half, half)
    for core in range(CORES):
        placed_ref[core, pl.ds(at, half), :] = turned[core * half : (core + 1) * half]


def project(place, stripes, everything, residual, gate):
    rows, outs = residual.shape
    sp = everything.shape[0]
    parts = 8
    vmem = pl.BlockSpec(memory_space=pltpu.VMEM)
    smem = pl.BlockSpec(memory_space=pltpu.SMEM)
    return pl.pallas_call(
        functools.partial(project_kernel, parts),
        out_shape=(
            jax.ShapeDtypeStruct((CORES, outs, rows), jnp.float32),
            jax.ShapeDtypeStruct((stripes.shape[0], outs + 16, rows), jnp.bfloat16),
        ),
        in_specs=[smem, vmem, pl.BlockSpec(memory_space=pltpu.HBM), vmem, vmem],
        out_specs=(vmem, vmem),
        scratch_shapes=[
            pltpu.VMEM((sp, CORES, outs // CORES, LANES), jnp.bfloat16),
            pltpu.SemaphoreType.DMA((parts,)),
        ],
        compiler_params=pltpu.CompilerParams(vmem_limit_bytes=LIMIT * MEBI),
        name="project",
    )(place, stripes, everything, residual, gate)


def feed_kernel(
    place_ref, messages_ref, scales_ref, gates_ref, placed_ref, weights_ref, shares_ref, ups, downs, sems
):
    _, sp, depth, up_width = ups.shape
    whole = downs.shape[3]
    pieces = whole // LANES
    tp_size, outs, rows = gates_ref.shape
    chips = tp_size // CORES
    half = outs // PAIR
    copies, slot = ([], [], []), 0
    for kind, (first, held, count) in enumerate(
        ((half, ups, pieces), (half + 2 * pieces * depth, ups, 1), (half + pieces * depth, downs, pieces))
    ):
        for core in range(CORES):
            for j in range(count):
                lanes = (pieces if kind == 1 else j) * LANES
                copies[kind].append(
                    pltpu.make_async_copy(
                        weights_ref.at[:, core, pl.ds(first + j * depth, depth), :],
                        held.at[core, :, :, pl.ds(lanes, LANES)],
                        sems.at[slot],
                    )
                )
                slot += 1
    ordered = []
    for core in range(CORES):
        ordered += [*copies[0][core * pieces : (core + 1) * pieces], copies[1][core]]
    for copy in [*ordered, *copies[2]]:
        copy.start()
    spreads = []
    for t in range(tp_size):
        for member in range(PAIR):
            source = member * chips + t // CORES
            mean = jnp.sum(
                messages_ref[source, outs : outs + 16, :].astype(jnp.float32),
                axis=0,
                keepdims=True,
            )
            start = t % CORES * half
            spreads.append(
                messages_ref[source, start : start + half, :].astype(jnp.float32) + mean
            )
    features = tp_size * outs
    row_mean = sum(jnp.sum(part, axis=0, keepdims=True) for part in spreads) / features
    centred = [part - row_mean for part in spreads]
    spread = sum(jnp.sum(part * part, axis=0, keepdims=True) for part in centred) / features
    factor = lax.rsqrt(spread + 1e-06)
    turned = jnp.concatenate([part * factor for part in centred], axis=0).T
    normed = (turned * (1.0 + scales_ref[1:2, :]) + scales_ref[0:1, :]).astype(jnp.bfloat16)
    active = []
    for core in range(CORES):
        for start in range(0, up_width, 2 * LANES):
            first = core * (pieces + 1) + start // LANES
            for copy in ordered[first : first + 2]:
                copy.wait()
            block = ups[core, :, :, start : start + 2 * LANES].reshape(sp * depth, -1)
            hidden = jnp.dot(normed, block, preferred_element_type=jnp.float32)
            active.append(jax.nn.gelu(hidden, approximate=True))
    lane = lax.broadcasted_iota(jnp.int32, (rows, LANES), 1)
    for core in range(CORES):
        tail = active[2 * core + 1]
        moved = jnp.where(lane < LANES // 2, 0.0, pltpu.roll(tail[:, LANES:], LANES // 2, 1))
        active[2 * core + 1] = jnp.concatenate([tail[:, :LANES], moved], axis=1)
    kept = jnp.concatenate([part.astype(jnp.bfloat16) for part in active], axis=1)
    for copy in copies[2]:
        copy.wait()
    each = sp // tp_size
    low = lax.broadcasted_iota(jnp.int32, (half, rows), 1) < rows // 2
    for t in range(tp_size):
        block = jnp.concatenate(
            [
                part.reshape(each * depth, -1)
                for core in range(CORES)
                for part in (
                    downs[core, t * each : (t + 1) * each],
                    ups[core, t * each : (t + 1) * each, :, whole:],
                )
            ],
            axis=1,
        )
        total = contract_last(block, kept)
        total = total * gates_ref[t]
        total = total + jnp.where(place_ref[0] == t // CORES, placed_ref[t % CORES], 0.0)
        top, bottom = total[:half], total[half:]
        shares_ref[0, t] = jnp.where(low, top, pltpu.roll(bottom, rows // 2, 1)).astype(
            jnp.bfloat16
        )
        shares_ref[1, t] = jnp.where(low, pltpu.roll(top, rows // 2, 1), bottom).astype(
            jnp.bfloat16
        )


def feed(place, messages, scales, gates, placed, everything, depth, units):
    tp_size, outs, rows = gates.shape
    sp = everything.shape[0]
    pieces = units // PAIR // LANES
    vmem = pl.BlockSpec(memory_space=pltpu.VMEM)
    smem = pl.BlockSpec(memory_space=pltpu.SMEM)
    return pl.pallas_call(
        feed_kernel,
        out_shape=jax.ShapeDtypeStruct((PAIR, tp_size, outs // PAIR, rows), jnp.bfloat16),
        in_specs=[smem, vmem, vmem, vmem, vmem, pl.BlockSpec(memory_space=pltpu.HBM)],
        out_specs=vmem,
        scratch_shapes=[
            pltpu.VMEM((CORES, sp, depth, (pieces + 1) * LANES), jnp.bfloat16),
            pltpu.VMEM((CORES, sp, depth, pieces * LANES), jnp.bfloat16),
            pltpu.SemaphoreType.DMA((CORES * (2 * pieces + 1),)),
        ],
        compiler_params=pltpu.CompilerParams(vmem_limit_bytes=LIMIT * MEBI),
        name="feed",
    )(place, messages, scales, gates, placed, everything)


def finish_kernel(shares_ref, out_ref):
    sources = shares_ref.shape[0]
    batches, span, _ = out_ref.shape
    for batch in range(batches):
        total = jnp.zeros(shares_ref.shape[1:], jnp.float32)
        for source in range(batch, sources, batches):
            total = total + shares_ref[source].astype(jnp.float32)
        rest = jnp.zeros((-total.shape[0] % LANES, total.shape[1]), jnp.float32)
        turned = jnp.concatenate([total, rest], axis=0).T[:, : total.shape[0]]
        both = jnp.concatenate([turned[k * span : (k + 1) * span] for k in range(PAIR)], axis=1)
        out_ref[batch] = both.astype(jnp.bfloat16)


def body(
    query_rows, key_rows, value_rows, residual, modulation, out_weight, up_weight, down_weight
):
    side, chip = lax.axis_index("member"), lax.axis_index("x")
    everything = gathered_weights(out_weight, up_weight, down_weight, side)
    tp = ("x", "core")
    tp_size = lax.axis_size(tp)
    batches, rows_block, local_width = residual.shape
    depth, units = up_weight.shape
    rows = PAIR * rows_block
    half = local_width // PAIR

    parts = residual.reshape(batches, rows_block, PAIR, half).transpose(2, 0, 1, 3)
    parts = lax.all_to_all(
        parts.reshape(PAIR * batches, rows_block, half), ("member", "core"), 0, 0, tiled=True
    )
    parts = parts.reshape(PAIR, CORES, rows_block, half).transpose(0, 2, 1, 3)
    residual_rows = parts.reshape(rows, CORES * half)
    rows_of_modulation = lax.all_gather(modulation, tp, axis=0, tiled=False)
    scales = jnp.swapaxes(rows_of_modulation[:, 1:3], 0, 1).reshape(2, -1)
    gates = jnp.broadcast_to(
        rows_of_modulation[:, 3][:, :, None], (tp_size, local_width, rows)
    )
    gate = lax.dynamic_slice_in_dim(rows_of_modulation[:, 0], chip * CORES, CORES, axis=0)
    gate = jnp.where(side == 0, gate[:, :half], gate[:, half:]).reshape(1, CORES * half)

    own = attend(query_rows, key_rows, value_rows)
    stripes = sent_to_all(own.reshape(-1, HEAD_FEATURES), ("member", "x"))
    place = jnp.stack([chip, side]).astype(jnp.int32)
    stripes, gates = lax.optimization_barrier((stripes, gates))
    placed, messages = project(place, stripes, everything, residual_rows, gate)
    messages = lax.all_to_all(messages, ("member", "x"), 0, 0, tiled=True)
    shares = feed(place, messages, scales, gates, placed, everything, depth, units)
    shares = shares.reshape(PAIR * tp_size, half, rows)
    shares = lax.all_to_all(shares, ("member", "x", "core"), 0, 0, tiled=True)
    return pl.pallas_call(
        finish_kernel,
        out_shape=jax.ShapeDtypeStruct(residual.shape, residual.dtype),
        compiler_params=pltpu.CompilerParams(vmem_limit_bytes=8 * MEBI),
        name="finish",
    )(shares)


def solution(mesh):
    groups, tp, sp = (mesh.shape[a] for a in ("groups", "tp", "sp"))
    fine = Mesh(
        mesh.devices.reshape(groups // PAIR, PAIR, tp // CORES, CORES, sp),
        ("pairs", "member", "x", "core", "sp"),
    )
    jobs, tokens, tensor = ("pairs", "member"), ("sp", "x", "core"), ("x", "core")
    in_specs = (
        P(jobs, tokens, None),
        P(jobs, tokens, None),
        P(jobs, tokens, None),
        P(jobs, "sp", tensor),
        P(None, tensor),
        P(tensor, "sp"),
        P("sp", tensor),
        P("sp", tensor),
    )
    out_specs = P(jobs, "sp", tensor)
    return jax.shard_map(body, mesh=fine, in_specs=in_specs, out_specs=out_specs, check_vma=False)
```
